8 devices in a mesh: dp: 2 (over y, z), tp: 4 (over x, core).
Axes of the slice: x: 2, y: 2, z: 1, core: 2. Of those that a mesh axis runs over, the one named last changes fastest.
Arguments:
- x: bfloat16 [8, 512, 5120], P('dp'), parts along dimension 0
- gain_a: bfloat16 [5120], replicated
- wq: bfloat16 [5120, 5120], P(None, 'tp')
- wk: bfloat16 [5120, 1024], P(None, 'tp')
- wv: bfloat16 [5120, 1024], P(None, 'tp')
- wo: bfloat16 [5120, 5120], P('tp')
- gain_m: bfloat16 [5120], replicated
- w_gate: bfloat16 [5120, 27648], P(None, 'tp')
- w_up: bfloat16 [5120, 27648], P(None, 'tp')
- w_down: bfloat16 [27648, 5120], P('tp')
Outputs:
- output: bfloat16 [8, 512, 5120], P('dp'), parts along dimension 0
There are 2 independent parts. The reference program is written for one: setup_inputs(seed, part) draws one part's arguments, and reference() takes and returns one part's arrays. A program takes and returns all parts, laid end to end along the dimension named above; an argument that names none is the same for every part.
All inputs are finite; a program needn't handle non-finite values.
Results may differ from the reference program's by a relative error of at most 0.017.
Values are sent between devices in bfloat16 or wider.
A program may use at most 2 GiB of HBM per device.

```python
import jax
import jax.numpy as jnp
from jax import lax

SEQUENCES = 4
TOKENS = 512
D = 5120
HEADS = 40
KV_HEADS = 8
HEAD = 128
FF = 27648
THETA = 10000


def setup_inputs(seed: int = 0, part: int = 0) -> dict:
    kx, ka, km, kq, kk, kv, ko, kg, ku, kd = jax.random.split(jax.random.key(seed), 10)

    def weights(key, rows, columns):
        return jax.random.normal(key, (rows, columns), jnp.float32) * rows**-0.5

    drawn = {
        "x": jax.random.normal(jax.random.fold_in(kx, part), (SEQUENCES, TOKENS, D), jnp.float32),
        "gain_a": 1 + 0.1 * jax.random.normal(ka, (D,), jnp.float32),
        "wq": 2 * weights(kq, D, HEADS * HEAD),
        "wk": 2 * weights(kk, D, KV_HEADS * HEAD),
        "wv": 4 * weights(kv, D, KV_HEADS * HEAD),
        "wo": weights(ko, HEADS * HEAD, D),
        "gain_m": 1 + 0.1 * jax.random.normal(km, (D,), jnp.float32),
        "w_gate": weights(kg, D, FF),
        "w_up": weights(ku, D, FF),
        "w_down": 3 * weights(kd, FF, D),
    }
    return {k: v.astype(jnp.bfloat16) for k, v in drawn.items()}


def normed(x, gain):
    wide = x.astype(jnp.float32)
    scale = lax.rsqrt(jnp.mean(wide * wide, -1, keepdims=True) + 1e-6)
    return (wide * scale * gain.astype(jnp.float32)).astype(jnp.bfloat16)


def turned(t, place, theta):
    half = t.shape[-1] // 2
    angle = place.astype(jnp.float32)[:, None] * theta ** (-jnp.arange(half, dtype=jnp.float32) / half)
    cos, sin = jnp.cos(angle)[:, None], jnp.sin(angle)[:, None]
    a, b = t[..., :half].astype(jnp.float32), t[..., half:].astype(jnp.float32)
    return jnp.concatenate([a * cos - b * sin, b * cos + a * sin], -1).astype(jnp.bfloat16)


def matmul(a, w):
    return jnp.dot(a, w, preferred_element_type=jnp.float32).astype(jnp.bfloat16)


def einsum(form, a, b):
    return jnp.einsum(form, a.astype(jnp.float32), b.astype(jnp.float32))


def attention(q, k, v):
    scores = einsum("tgsd,ugd->gstu", q, k) * q.shape[-1] ** -0.5
    token = jnp.arange(q.shape[0])
    scores = jnp.where(token[:, None] >= token, scores, -jnp.inf)
    weights = jax.nn.softmax(scores, -1).astype(jnp.bfloat16)
    return einsum("gstu,ugd->tgsd", weights, v).astype(jnp.bfloat16)


def one(x, gain_a, wq, wk, wv, wo, gain_m, w_gate, w_up, w_down):
    rows = x.shape[0]
    a, place = normed(x, gain_a), jnp.arange(rows)
    k = turned(matmul(a, wk).reshape(rows, -1, HEAD), place, THETA)
    q = turned(matmul(a, wq).reshape(rows, -1, HEAD), place, THETA).reshape(rows, k.shape[1], -1, HEAD)
    v = matmul(a, wv).reshape(rows, -1, HEAD)
    seen = attention(q, k, v).reshape(rows, -1)
    h = (x.astype(jnp.float32) + jnp.dot(seen, wo, preferred_element_type=jnp.float32)).astype(jnp.bfloat16)
    b = normed(h, gain_m)
    gate = jnp.dot(b, w_gate, preferred_element_type=jnp.float32)
    up = jnp.dot(b, w_up, preferred_element_type=jnp.float32)
    hidden = (jax.nn.silu(gate) * up).astype(jnp.bfloat16)
    return (h.astype(jnp.float32) + jnp.dot(hidden, w_down, preferred_element_type=jnp.float32)).astype(jnp.bfloat16)


def reference(x, gain_a, wq, wk, wv, wo, gain_m, w_gate, w_up, w_down):
    return lax.map(lambda sequence: one(sequence, gain_a, wq, wk, wv, wo, gain_m, w_gate, w_up, w_down), x)
```

```python
import functools

import jax
import jax.numpy as jnp
from jax import lax
from jax.experimental import pallas as pl
from jax.experimental.pallas import tpu as pltpu
from jax.sharding import PartitionSpec as P


HEAD = 128
THETA = 10000
LOG2E = 1.4426950408889634
EPS = 1e-6
VMEM = 62 * 2**20
ROWS = 32


def _call(kernel, token, given, grid, in_specs, out_specs, out_shape, scratch=(), aliases=None, cost=None, vmem=VMEM):
    n, m = len(in_specs), len(out_specs)

    def body(*refs):
        kernel(*refs[: 1 + n], *refs[2 + n : 2 + n + m], *refs[3 + n + m :])

    anywhere = pl.BlockSpec(memory_space=pl.ANY)
    out = pl.pallas_call(
        body,
        grid_spec=pltpu.PrefetchScalarGridSpec(num_scalar_prefetch=1, grid=grid, in_specs=[*in_specs, anywhere], out_specs=[*out_specs, anywhere],
                                               scratch_shapes=list(scratch)),
        out_shape=[*out_shape, jax.ShapeDtypeStruct((8, 128), jnp.float32)],
        input_output_aliases=aliases or {},
        compiler_params=pltpu.CompilerParams(dimension_semantics=("arbitrary",), vmem_limit_bytes=vmem),
        cost_estimate=cost,
    )(*given, token)
    return out[:-1], out[-1]


def _dot(a, b, ca=1, cb=0):
    return lax.dot_general(a, b, (((ca,), (cb,)), ((), ())), preferred_element_type=jnp.float32)


def _once(shape, index_map):
    return pl.BlockSpec(shape, index_map, pipeline_mode=pl.Buffered(1))


def _rotate(t, cos, sin):
    t = t.astype(jnp.float32)
    return (t * cos + pltpu.roll(t, HEAD // 2, 1) * sin).astype(jnp.bfloat16)


def _one_head(q, k, vt, o_ref, at, tokens):
    e = HEAD**-0.5 * LOG2E
    half = tokens // 2
    for i in range(2):
        n = half * (i + 1)
        s = _dot(k[:n], q[half * i : n], 1, 1)
        key = lax.broadcasted_iota(jnp.int32, (half, half), 0)
        query = lax.broadcasted_iota(jnp.int32, (half, half), 1)
        last = jnp.where(query >= key, s[n - half :], -1e30)
        if i:
            s = jnp.concatenate([s[:half], last], 0)
        else:
            s = last
        top = s.max(axis=0, keepdims=True)
        p = jnp.exp2((s - top) * e).astype(jnp.bfloat16)
        mix = _dot(vt[:, :n], p)
        o = mix[:HEAD] * (1 / mix[HEAD : HEAD + 1])
        o_ref[half * i : n, pl.ds(at, HEAD)] = o.T.astype(jnp.bfloat16)


def _attention_kernel(pos_ref, x_ref, gain_ref, cos_ref, sin_ref, wk_ref, wv_ref, wq_ref, wo_ref, send_ref, keep_ref,
                      a_s, q_s, k_s, vt_s, seen_s, *, nq, group, per):
    j = pl.program_id(0)
    tokens, d = a_s.shape
    kvs = k_s.shape[0]

    @pl.when(j == 0)
    def _():
        def rows(r, _):
            at = pl.ds(pl.multiple_of(r * ROWS, ROWS), ROWS)
            wide = x_ref[0, at, :].astype(jnp.float32)
            scale = lax.rsqrt(jnp.mean(wide * wide, -1, keepdims=True) + EPS)
            a_s[at, :] = (wide * scale * gain_ref[...].astype(jnp.float32)).astype(jnp.bfloat16)
            return _

        lax.fori_loop(0, tokens // ROWS, rows, None)
        t = _dot(a_s[...], wk_ref[...]).astype(jnp.bfloat16)
        for i in range(kvs):
            k_s[i] = _rotate(t[:, i * HEAD : (i + 1) * HEAD], cos_ref[...], sin_ref[...])

    @pl.when(j == 1)
    def _():
        t = _dot(a_s[...], wv_ref[...])
        for i in range(kvs):
            vt_s[i, :HEAD, :] = t[:, i * HEAD : (i + 1) * HEAD].T.astype(jnp.bfloat16)
            vt_s[i, HEAD:, :] = jnp.ones((16, tokens), jnp.bfloat16)

    def project(i):
        t = _dot(a_s[...], wq_ref[...]).astype(jnp.bfloat16)
        for n in range(2):
            q_s[lax.rem(i, 2), n] = _rotate(t[:, n * HEAD : (n + 1) * HEAD], cos_ref[...], sin_ref[...])

    def attend(i):
        for n in range(2):
            head = 2 * i + n
            kv = lax.div(head, group)
            _one_head(q_s[lax.rem(i, 2), n], k_s[kv], vt_s[kv], seen_s, pl.multiple_of(head * HEAD, HEAD), tokens)

    @pl.when(j == 2)
    def _():
        project(0)

    @pl.when((j > 2) & (j < 2 + nq))
    def _():
        attend(j - 3)
        project(j - 2)

    @pl.when(j == 2 + nq)
    def _():
        attend(nq - 1)

    @pl.when(j > 2 + nq)
    def _():
        term = _dot(seen_s[...], wo_ref[...]).astype(jnp.bfloat16)

        @pl.when(j < 3 + nq + per)
        def _():
            send_ref[...] = term

        @pl.when(j >= 3 + nq + per)
        def _():
            keep_ref[...] = term


def attention_half(token, pos, x, gain, cos, sin, wk, wv, wq, wo):
    _, tokens, d = x.shape
    qd, kvd = wq.shape[1], wk.shape[1]
    nq, wide, half = qd // 256, 1280, d // 2
    per = half // wide
    first = 3 + nq

    def out_column(j, pos):
        n = jnp.maximum(j - first, 0)
        return jnp.where(n < per, (1 - pos[0]) * per + n, pos[0] * per + n - per)

    whole = lambda j, pos: (0, 0)
    out = jax.ShapeDtypeStruct((tokens, half), jnp.bfloat16)
    return _call(
        functools.partial(_attention_kernel, nq=nq, group=qd // kvd, per=per), token, (pos, x, gain, cos, sin, wk, wv, wq, wo), (first + 2 * per,),
        in_specs=[
            _once((1, tokens, d), lambda j, pos: (pos[1], 0, 0)),
            _once((1, d), whole),
            _once((tokens, HEAD), whole),
            _once((tokens, HEAD), whole),
            _once((d, kvd), whole),
            _once((d, kvd), whole),
            pl.BlockSpec((d, 256), lambda j, pos: (0, jnp.clip(j - 2, 0, nq - 1))),
            pl.BlockSpec((qd, wide), lambda j, pos: (0, out_column(j, pos))),
        ],
        out_specs=[
            pl.BlockSpec((tokens, wide), lambda j, pos: (0, jnp.clip(j - first, 0, per - 1))),
            pl.BlockSpec((tokens, wide), lambda j, pos: (0, jnp.clip(j - first - per, 0, per - 1))),
        ],
        out_shape=[out, out],
        scratch=[
            pltpu.VMEM((tokens, d), jnp.bfloat16),
            pltpu.VMEM((2, 2, tokens, HEAD), jnp.bfloat16),
            pltpu.VMEM((kvd // HEAD, tokens, HEAD), jnp.bfloat16),
            pltpu.VMEM((kvd // HEAD, HEAD + 16, tokens), jnp.bfloat16),
            pltpu.VMEM((tokens, qd), jnp.bfloat16),
        ],
        cost=pl.CostEstimate(
            flops=2 * tokens * d * (2 * qd + 2 * kvd) + 4 * tokens * tokens * qd, transcendentals=tokens * tokens * qd // HEAD,
            bytes_accessed=2 * (2 * tokens * d + d * (2 * qd + 2 * kvd))),
    )


def _mlp_kernel(pos_ref, own_ref, sib_ref, gain_ref, wg_ref, wu_ref, wd_ref, send_ref, keep_ref, b_s, hid_s, *, nf, per):
    j = pl.program_id(0)
    tokens, d = b_s.shape
    half, bn = d // 2, wg_ref.shape[1]

    @pl.when(j == 0)
    def _():
        mine = pl.ds(pl.multiple_of(pos_ref[0] * half, half), half)
        other = pl.ds(pl.multiple_of((1 - pos_ref[0]) * half, half), half)

        def rows(r, _):
            at = pl.ds(pl.multiple_of(r * ROWS, ROWS), ROWS)
            own, sib = own_ref[at, :].astype(jnp.float32), sib_ref[at, :].astype(jnp.float32)
            total = jnp.sum(own * own, -1, keepdims=True) + jnp.sum(sib * sib, -1, keepdims=True)
            scale = lax.rsqrt(total * (1 / d) + EPS)
            b_s[at, mine] = (own * scale * gain_ref[:, mine].astype(jnp.float32)).astype(jnp.bfloat16)
            b_s[at, other] = (sib * scale * gain_ref[:, other].astype(jnp.float32)).astype(jnp.bfloat16)
            return _

        lax.fori_loop(0, tokens // ROWS, rows, None)

    @pl.when(j < nf)
    def _():
        gate, up = _dot(b_s[...], wg_ref[...]), _dot(b_s[...], wu_ref[...])
        hid_s[:, pl.ds(pl.multiple_of(j * bn, bn), bn)] = (gate * jax.nn.sigmoid(gate) * up).astype(jnp.bfloat16)

    @pl.when(j >= nf)
    def _():
        term = _dot(hid_s[...], wd_ref[...]).astype(jnp.bfloat16)

        @pl.when(j < nf + per)
        def _():
            send_ref[...] = term

        @pl.when(j >= nf + per)
        def _():
            keep_ref[...] = term


def mlp(token, pos, own, sib, gain, wg, wu, wd, bn=384, bd=512):
    tokens, half = own.shape
    d, ff = wg.shape
    nf, per = ff // bn, half // bd

    def out_column(j, pos):
        n = jnp.maximum(j - nf, 0)
        return jnp.where(n < per, (1 - pos[0]) * per + n, pos[0] * per + n - per)

    whole = lambda j, pos: (0, 0)
    out = jax.ShapeDtypeStruct((tokens, half), jnp.bfloat16)
    return _call(
        functools.partial(_mlp_kernel, nf=nf, per=per), token, (pos, own, sib, gain, wg, wu, wd), (nf + 2 * per,),
        in_specs=[
            _once((tokens, half), whole),
            _once((tokens, half), whole),
            _once((1, d), whole),
            pl.BlockSpec((d, bn), lambda j, pos: (0, jnp.minimum(j, nf - 1))),
            pl.BlockSpec((d, bn), lambda j, pos: (0, jnp.minimum(j, nf - 1))),
            pl.BlockSpec((ff, bd), lambda j, pos: (0, out_column(j, pos))),
        ],
        out_specs=[
            pl.BlockSpec((tokens, bd), lambda j, pos: (0, jnp.clip(j - nf, 0, per - 1))),
            pl.BlockSpec((tokens, bd), lambda j, pos: (0, jnp.clip(j - nf - per, 0, per - 1))),
        ],
        out_shape=[out, out],
        scratch=[pltpu.VMEM((tokens, d), jnp.bfloat16), pltpu.VMEM((tokens, ff), jnp.bfloat16)],
        cost=pl.CostEstimate(flops=6 * tokens * d * ff, transcendentals=tokens * ff, bytes_accessed=2 * (3 * d * ff + 2 * tokens * d)),
    )


def _add_kernel(pos_ref, *refs):
    *terms, o_ref = refs
    total = None
    for t in terms[::-1]:
        t = t[...].reshape(o_ref.shape).astype(jnp.float32)
        total = t if total is None else t + total
    o_ref[...] = total.astype(jnp.bfloat16)


def add(token, pos, *terms):
    tokens, half = terms[-1].shape
    rows = min(tokens, 128)
    flat = pl.BlockSpec((rows, half), lambda j, pos: (j, 0))
    deep = pl.BlockSpec((1, rows, half), lambda j, pos: (pos[1], j, pos[0]))
    (out,), token = _call(
        _add_kernel, token, (pos, *terms), (tokens // rows,),
        in_specs=[flat if t.ndim == 2 else deep for t in terms],
        out_specs=[flat],
        out_shape=[jax.ShapeDtypeStruct((tokens, half), jnp.bfloat16)],
        cost=pl.CostEstimate(flops=len(terms) * tokens * half, transcendentals=0, bytes_accessed=2 * (len(terms) + 1) * tokens * half),
    )
    return out, token


def _place_kernel(pos_ref, own_ref, sib_ref, *rest):
    o_ref = rest[-1]
    mine = pl.program_id(0) == pos_ref[0]

    @pl.when(mine)
    def _():
        o_ref[0] = own_ref[...]

    @pl.when(jnp.logical_not(mine))
    def _():
        o_ref[0] = sib_ref[...]


def place(token, pos, own, sib, result, shape):
    tokens, half = own.shape
    given = [] if result is None else [result]
    (out,), token = _call(
        _place_kernel, token, (pos, own, sib, *given), (2,),
        in_specs=[_once((tokens, half), lambda j, pos: (0, 0))] * 2 + [pl.BlockSpec(memory_space=pl.ANY)] * len(given),
        out_specs=[pl.BlockSpec((1, tokens, half), lambda j, pos: (pos[1], 0, j))],
        out_shape=[jax.ShapeDtypeStruct(shape, jnp.bfloat16)],
        aliases={3: 0} if given else None,
        cost=pl.CostEstimate(flops=tokens * half, transcendentals=0, bytes_accessed=8 * tokens * half),
    )
    return out, token


ORDER = (
    "A0", "A1", "SA0", "A2", "SA1", "A3", "SA2", "H0", "SA3", "M0", "H1", "SM0", "H2", "M1", "H3", "SM1", "M2",
    "R0", "SM2", "R1", "P0", "P1", "M3", "R2", "SM3", "P2", "R3", "P3",
)


def solution(mesh):
    n = mesh.shape["tp"]
    core_pairs = [(i, i ^ 1) for i in range(n)]
    chip_pairs = [(i, i ^ 2) for i in range(n)]

    def step(x, gain_a, wq, wk, wv, wo, gain_m, w_gate, w_up, w_down):
        tokens, d = x.shape[1:]
        core = lax.rem(lax.axis_index("tp"), 2)
        pos = [jnp.stack([core, jnp.int32(s)]) for s in range(4)]
        angle = jnp.arange(tokens, dtype=jnp.float32)[:, None] * THETA ** (-jnp.arange(HEAD // 2, dtype=jnp.float32) / (HEAD // 2))
        cos, sin = jnp.cos(angle), jnp.sin(angle)
        cos, sin = jnp.concatenate([cos, cos], -1), jnp.concatenate([-sin, sin], -1)
        gain_a, gain_m = gain_a.reshape(1, d), gain_m.reshape(1, d)
        token, y, made, came = jnp.zeros((8, 128), jnp.float32), None, {}, {}

        for op in ORDER:
            kind, s = op[:-1], op[-1]
            at = pos[int(s)]
            if kind == "A":
                (send, made[op]), token = attention_half(token, at, x, gain_a, cos, sin, wk, wv, wq, wo)
            elif kind == "M":
                (send, made[op]), token = mlp(token, at, made["H" + s], came["H" + s], gain_m, w_gate, w_up, w_down)
            elif kind in ("SA", "SM"):
                made[op], token = add(token, at, made[kind[1] + s], came[kind[1] + s])
            elif kind in ("H", "R"):
                base, term = (x, "SA" + s) if kind == "H" else (made["H" + s], "SM" + s)
                made[op], token = add(token, at, base, made[term], came[term])
            else:
                y, token = place(token, at, made["R" + s], came["R" + s], y, x.shape)
            if kind != "P":
                pairs = chip_pairs if kind in ("SA", "SM") else core_pairs
                came[op] = lax.ppermute(send if kind in ("A", "M") else made[op], "tp", pairs)
        return y

    tokens, whole, columns, rows_of = P("dp", None, None), P(None), P(None, "tp"), P("tp", None)
    return jax.shard_map(
        step,
        mesh=mesh,
        in_specs=(tokens, whole, columns, columns, columns, rows_of, whole, columns, columns, rows_of),
        out_specs=tokens,
        check_vma=False,
    )
```

```python
import functools

import jax
import jax.numpy as jnp
from jax import lax
from jax.experimental import pallas as pl
from jax.experimental.pallas import tpu as pltpu
from jax.sharding import PartitionSpec as P


HEAD = 128
THETA = 10000
LOG2E = 1.4426950408889634
EPS = 1e-6
VMEM = 66_500_000
PANEL = 256
PIECE = 1280

ANY = pl.BlockSpec(memory_space=pl.ANY)


def _call(kernel, token, given, grid, in_specs, out_specs, out_shape, scratch=(), aliases=None, cost=None):
    n, m = len(in_specs), len(out_specs)

    def body(*refs):
        kernel(*refs[: 1 + n], *refs[2 + n : 2 + n + m], *refs[3 + n + m :])

    out = pl.pallas_call(
        body,
        grid_spec=pltpu.PrefetchScalarGridSpec(num_scalar_prefetch=1, grid=grid, in_specs=[*in_specs, ANY], out_specs=[*out_specs, ANY],
                                               scratch_shapes=list(scratch)),
        out_shape=[*out_shape, jax.ShapeDtypeStruct((8, 128), jnp.float32)],
        input_output_aliases=aliases or {},
        compiler_params=pltpu.CompilerParams(dimension_semantics=("arbitrary",) * len(grid), vmem_limit_bytes=VMEM),
        cost_estimate=cost,
    )(*given, token)
    return out[:-1], out[-1]


def _dot(a, b, ca=1, cb=0):
    return lax.dot_general(a, b, (((ca,), (cb,)), ((), ())), preferred_element_type=jnp.float32)


def _once(shape, index_map):
    return pl.BlockSpec(shape, index_map, pipeline_mode=pl.Buffered(1))


def _norm(x_ref, gain_ref, o_ref, column, rows=64):
    tokens, d = o_ref.shape

    def some(r, _):
        at = pl.ds(pl.multiple_of(r * rows, rows), rows)
        total = jnp.zeros((rows, 128), jnp.float32)
        for c in range(d // 128):
            wide = x_ref[at, c * 128 : (c + 1) * 128].astype(jnp.float32)
            total += wide * wide
        scale = lax.rsqrt(jnp.sum(total, -1, keepdims=True) * (1 / d) + EPS)
        for c in range(d // 128):
            to = pl.ds(pl.multiple_of(column(c), 128), 128)
            wide = x_ref[at, c * 128 : (c + 1) * 128].astype(jnp.float32)
            o_ref[at, to] = (wide * scale * gain_ref[:, to].astype(jnp.float32)).astype(jnp.bfloat16)
        return _

    lax.fori_loop(0, tokens // rows, some, None)


def _rotate(t, cos, sin):
    t = t.astype(jnp.float32)
    return (t * cos + pltpu.roll(t, HEAD // 2, 1) * sin).astype(jnp.bfloat16)


def _one_head(q, k, vt, o_ref, at, tokens):
    e = HEAD**-0.5 * LOG2E
    half = tokens // 2
    for i in range(2):
        n = half * (i + 1)
        s = _dot(k[:n], q[half * i : n], 1, 1)
        key = lax.broadcasted_iota(jnp.int32, (half, half), 0)
        query = lax.broadcasted_iota(jnp.int32, (half, half), 1)
        last = jnp.where(query >= key, s[n - half :], -1e30)
        s = jnp.concatenate([s[:half], last], 0) if i else last
        top = s.max(axis=0, keepdims=True)
        p = jnp.exp2((s - top) * e).astype(jnp.bfloat16)
        mix = _dot(vt[:, :n], p)
        o = mix[:HEAD] * (1 / mix[HEAD : HEAD + 1])
        o_ref[half * i : n, pl.ds(at, HEAD)] = o.T.astype(jnp.bfloat16)


def _attention_kernel(pos_ref, x_hbm, gain_ref, cos_ref, sin_ref, wk_hbm, wv_hbm, wq_hbm, wo_hbm, send_ref, keep_ref,
                      x_s, a_s, q_s, k_s, vt_s, seen_s, w_s, wo_s, x_sem, w_sem, *, group):
    i = pl.program_id(0)
    tokens, d = a_s.shape
    kvs, nq, no = k_s.shape[0], w_s.shape[0] - 2, wo_s.shape[0]
    per = no // 2

    def fetch(n):
        return pltpu.make_async_copy(x_hbm.at[pos_ref[1] + n], x_s, x_sem)

    def weight(n):
        if isinstance(n, int) and n < 2:
            src = (wk_hbm, wv_hbm)[n]
        else:
            src = wq_hbm.at[:, pl.ds(pl.multiple_of((n - 2) * PANEL, PANEL), PANEL)]
        return pltpu.make_async_copy(src, w_s.at[n], w_sem.at[n])

    def out_weight(n):
        half = (1 - pos_ref[0]) if n < per else pos_ref[0]
        column = pl.multiple_of((half * per + n % per) * PIECE, PIECE)
        return pltpu.make_async_copy(wo_hbm.at[:, pl.ds(column, PIECE)], wo_s.at[n], w_sem.at[2 + nq + n])

    def ready(copy):
        @pl.when(i == 0)
        def _():
            copy.wait()

    @pl.when(i == 0)
    def _():
        fetch(0).start()
        for n in range(2 + nq):
            weight(n).start()
        for n in range(no):
            out_weight(n).start()

    fetch(i).wait()
    _norm(x_s, gain_ref, a_s, lambda c: c * 128)

    @pl.when(i + 1 < pl.num_programs(0))
    def _():
        fetch(i + 1).start()

    def project(r):
        t = _dot(a_s[...], w_s[r + 2]).astype(jnp.bfloat16)
        for n in range(2):
            q_s[lax.rem(r, 2), n] = _rotate(t[:, n * HEAD : (n + 1) * HEAD], cos_ref[...], sin_ref[...])

    def attend(r):
        for n in range(2):
            head = 2 * r + n
            kv = lax.div(head, group)
            _one_head(q_s[lax.rem(r, 2), n], k_s[kv], vt_s[kv], seen_s, pl.multiple_of(head * HEAD, HEAD), tokens)

    for n in range(3):
        ready(weight(n))
    t = _dot(a_s[...], w_s[0]).astype(jnp.bfloat16)
    for n in range(kvs):
        k_s[n] = _rotate(t[:, n * HEAD : (n + 1) * HEAD], cos_ref[...], sin_ref[...])
    t = _dot(a_s[...], w_s[1])
    for n in range(kvs):
        vt_s[n, :HEAD, :] = t[:, n * HEAD : (n + 1) * HEAD].T.astype(jnp.bfloat16)
        vt_s[n, HEAD:, :] = jnp.ones((16, tokens), jnp.bfloat16)
    project(jnp.int32(0))

    def both(r, _):
        ready(weight(r + 3))
        attend(r)
        project(r + 1)
        return _

    lax.fori_loop(0, nq - 1, both, None)
    attend(jnp.int32(nq - 1))
    for n in range(no):
        ready(out_weight(n))
    for n in range(no):
        o_ref = send_ref if n < per else keep_ref
        o_ref[:, n % per * PIECE : (n % per + 1) * PIECE] = _dot(seen_s[...], wo_s[n]).astype(jnp.bfloat16)


def attention_half(token, pos, x, gain, cos, sin, wk, wv, wq, wo, count):
    _, tokens, d = x.shape
    qd, kvd, half = wq.shape[1], wk.shape[1], d // 2
    nq, no = qd // PANEL, d // PIECE
    whole = lambda i, pos: (0, 0)
    out = jax.ShapeDtypeStruct((count * tokens, half), jnp.bfloat16)
    rows = pl.BlockSpec((tokens, half), lambda i, pos: (i, 0))
    return _call(
        functools.partial(_attention_kernel, group=qd // kvd), token, (pos, x, gain, cos, sin, wk, wv, wq, wo), (count,),
        in_specs=[ANY, _once((1, d), whole), _once((tokens, HEAD), whole), _once((tokens, HEAD), whole), ANY, ANY, ANY, ANY],
        out_specs=[rows, rows],
        out_shape=[out, out],
        scratch=[
            pltpu.VMEM((tokens, d), jnp.bfloat16),
            pltpu.VMEM((tokens, d), jnp.bfloat16),
            pltpu.VMEM((2, 2, tokens, HEAD), jnp.bfloat16),
            pltpu.VMEM((kvd // HEAD, tokens, HEAD), jnp.bfloat16),
            pltpu.VMEM((kvd // HEAD, HEAD + 16, tokens), jnp.bfloat16),
            pltpu.VMEM((tokens, qd), jnp.bfloat16),
            pltpu.VMEM((2 + nq, d, PANEL), jnp.bfloat16),
            pltpu.VMEM((no, qd, PIECE), jnp.bfloat16),
            pltpu.SemaphoreType.DMA,
            pltpu.SemaphoreType.DMA((2 + nq + no,)),
        ],
        cost=pl.CostEstimate(
            flops=count * (2 * tokens * d * (2 * qd + 2 * kvd) + 4 * tokens * tokens * qd),
            transcendentals=count * tokens * tokens * qd // HEAD,
            bytes_accessed=2 * (2 * count * tokens * d + d * (2 * qd + 2 * kvd))),
    )


def _mlp_kernel(pos_ref, *refs, nf, pieces, hidden_in, hidden_out):
    if hidden_in:
        hid_hbm, wd_hbm, send_hbm, keep_hbm, w_s, hid_s, t_s, w_sem, h_sem, t_sem = refs
    elif hidden_out:
        own_hbm, sib_hbm, gain_ref, wg_hbm, wu_hbm, wd_hbm, send_hbm, keep_hbm, hid_hbm, w_s, b_s, hid_s, t_s, w_sem, h_sem, t_sem = refs
    else:
        own_hbm, sib_hbm, gain_ref, wg_hbm, wu_hbm, wd_hbm, send_hbm, keep_hbm, w_s, b_s, hid_s, t_s, w_sem, h_sem, t_sem = refs
    j = pl.program_id(0)
    slot = lax.rem(j, 2)
    tokens, ff = hid_s.shape
    half = wd_hbm.shape[1] // 2
    per, npan, last = len(pieces), PIECE // PANEL, nf + 2 * len(pieces)
    bn = 3 * PANEL

    def gate_up(i, step, slot):
        src = (wg_hbm, wu_hbm)[i % 2]
        d = src.shape[0]
        column = pl.multiple_of(step * bn + i // 2 * PANEL, PANEL)
        return pltpu.make_async_copy(src.at[:, pl.ds(column, PANEL)], w_s.at[slot, pl.ds(i * d, d), :], w_sem.at[slot, i])

    def down(i, step, slot):
        n = step - nf
        core = jnp.where(n < per, 1 - pos_ref[0], pos_ref[0])
        piece = lax.rem(n, per) + pieces[0]
        column = pl.multiple_of(core * half + piece * PIECE + i * PANEL, PANEL)
        return pltpu.make_async_copy(wd_hbm.at[:, pl.ds(column, PANEL)], w_s.at[slot, pl.ds(i * ff, ff), :], w_sem.at[slot, i])

    def start(step, slot):
        if nf:
            @pl.when(step < nf)
            def _():
                for i in range(6):
                    gate_up(i, step, slot).start()

        @pl.when((step >= nf) & (step < last))
        def _():
            for i in range(npan):
                down(i, step, slot).start()

    def out(n, slot, start):
        to = pl.multiple_of(lax.rem(n, per) * PIECE, PIECE)
        for ref, now in ((send_hbm, n < per), (keep_hbm, n >= per)):
            @pl.when(now)
            def _():
                copy = pltpu.make_async_copy(t_s.at[slot], ref.at[:, pl.ds(to, PIECE)], t_sem.at[slot])
                copy.start() if start else copy.wait()

    if hidden_in:
        first = [pltpu.make_async_copy(hid_hbm, hid_s, h_sem.at[0])]
    else:
        at = pl.ds(pl.multiple_of(pos_ref[2] * tokens, tokens), tokens)
        first = [pltpu.make_async_copy(own_hbm.at[at], hid_s.at[:, pl.ds(0, half)], h_sem.at[0]),
                 pltpu.make_async_copy(sib_hbm.at[at], hid_s.at[:, pl.ds(half, half)], h_sem.at[1])]

    @pl.when(j == 0)
    def _():
        for copy in first:
            copy.start()
        start(0, 0)

    start(j + 1, 1 - slot)

    @pl.when(j == 0)
    def _():
        for copy in first:
            copy.wait()
        if not hidden_in:
            d = 2 * half
            shift = pos_ref[0] * half
            _norm(hid_s, gain_ref, b_s, lambda c: lax.rem(shift + c * 128, d))

    if nf:
        @pl.when(j < nf)
        def _():
            for i in range(6):
                gate_up(i, j, slot).wait()
            d = b_s.shape[1]
            for p in range(3):
                gate = _dot(b_s[...], w_s[slot, 2 * p * d : (2 * p + 1) * d, :])
                up = _dot(b_s[...], w_s[slot, (2 * p + 1) * d : (2 * p + 2) * d, :])
                at = pl.ds(pl.multiple_of(j * bn + p * PANEL, PANEL), PANEL)
                hid_s[:, at] = (gate * jax.nn.sigmoid(gate) * up).astype(jnp.bfloat16)

    if hidden_out:
        put = pltpu.make_async_copy(hid_s, hid_hbm, h_sem.at[0])

        @pl.when(j == nf)
        def _():
            put.start()

    @pl.when(j >= nf)
    def _():
        n = j - nf
        spot = lax.rem(n, 2)

        @pl.when(n >= 2)
        def _():
            out(n - 2, spot, False)

        if not hidden_in:
            for i in range(npan):
                down(i, j, slot).wait()
        for i in range(npan):
            if hidden_in:
                down(i, j, slot).wait()
            t_s[spot, :, i * PANEL : (i + 1) * PANEL] = _dot(hid_s[...], w_s[slot, i * ff : (i + 1) * ff, :]).astype(jnp.bfloat16)
        out(n, spot, True)

        @pl.when(j == last - 1)
        def _():
            out(n - 1, 1 - spot, False)
            out(n, spot, False)
            if hidden_out:
                put.wait()


def mlp(token, pos, given, wd, pieces, hidden_out=False):
    ff, d = wd.shape
    tokens, hidden_in = 512, len(given) == 1
    per = len(pieces)
    nf = 0 if hidden_in else ff // (3 * PANEL)
    out = jax.ShapeDtypeStruct((tokens, per * PIECE), jnp.bfloat16)
    hidden = jax.ShapeDtypeStruct((tokens, ff), jnp.bfloat16)
    flops = (0 if hidden_in else 4 * tokens * d * ff) + 2 * tokens * ff * 2 * per * PIECE
    return _call(
        functools.partial(_mlp_kernel, nf=nf, pieces=pieces, hidden_in=hidden_in, hidden_out=hidden_out), token, (pos, *given, wd), (nf + 2 * per,),
        in_specs=[ANY, ANY] if hidden_in else [ANY, ANY, _once((1, d), lambda j, pos: (0, 0)), ANY, ANY, ANY],
        out_specs=[ANY] * (2 + hidden_out),
        out_shape=[out, out] + [hidden] * hidden_out,
        scratch=[pltpu.VMEM((2, max(6 * d, PIECE // PANEL * ff), PANEL), jnp.bfloat16)]
        + [pltpu.VMEM((tokens, d), jnp.bfloat16)] * (not hidden_in)
        + [
            pltpu.VMEM((tokens, ff), jnp.bfloat16),
            pltpu.VMEM((2, tokens, PIECE), jnp.bfloat16),
            pltpu.SemaphoreType.DMA((2, 6)),
            pltpu.SemaphoreType.DMA((2,)),
            pltpu.SemaphoreType.DMA((2,)),
        ],
        cost=pl.CostEstimate(flops=flops, transcendentals=tokens * ff, bytes_accessed=flops // tokens + 4 * tokens * d),
    )


def _add_kernel(pos_ref, *refs):
    *terms, o_ref = refs
    total = None
    for t in terms[::-1]:
        t = t[...].reshape(o_ref.shape).astype(jnp.float32)
        total = t if total is None else t + total
    o_ref[...] = total.astype(jnp.bfloat16)


def add(token, pos, *terms, rows=128):
    size, wide = terms[-1][0].shape
    per = 512 // rows

    def spec(array, row=0, column=0):
        if array.ndim == 3:
            return pl.BlockSpec((1, rows, wide), lambda j, pos: (pos[1] + j // per, lax.rem(j, per), pos[0]))
        return pl.BlockSpec((rows, wide), lambda j, pos: (row // rows + j, column // wide))

    (out,), token = _call(
        _add_kernel, token, (pos, *(t[0] for t in terms)), (size // rows,),
        in_specs=[spec(*t) for t in terms],
        out_specs=[spec(terms[-1][0])],
        out_shape=[jax.ShapeDtypeStruct((size, wide), jnp.bfloat16)],
        cost=pl.CostEstimate(flops=len(terms) * size * wide, transcendentals=0, bytes_accessed=2 * (len(terms) + 1) * size * wide),
    )
    return out, token


def _place_kernel(pos_ref, own_ref, sib_ref, *rest):
    o_ref = rest[-1]

    @pl.when(pl.program_id(1) == 0)
    def _():
        o_ref[0] = own_ref[...]

    @pl.when(pl.program_id(1) == 1)
    def _():
        o_ref[0] = sib_ref[...]


def place(token, pos, own, sib, result, shape, piece=0, rows=128):
    tokens, wide = own.shape
    per = shape[2] // 2 // wide
    given = [] if result is None else [result]
    block = pl.BlockSpec((rows, wide), lambda j, h, pos: (j, 0))
    (out,), token = _call(
        _place_kernel, token, (pos, own, sib, *given), (tokens // rows, 2),
        in_specs=[block, block] + [ANY] * len(given),
        out_specs=[pl.BlockSpec((1, rows, wide), lambda j, h, pos: (pos[1], j, jnp.where(h == 0, pos[0], 1 - pos[0]) * per + piece))],
        out_shape=[jax.ShapeDtypeStruct(shape, jnp.bfloat16)],
        aliases={3: 0} if given else None,
        cost=pl.CostEstimate(flops=tokens * wide, transcendentals=0, bytes_accessed=8 * tokens * wide),
    )
    return out, token


def solution(mesh):
    n = mesh.shape["tp"]
    core_pairs = [(i, i ^ 1) for i in range(n)]
    chip_pairs = [(i, i ^ 2) for i in range(n)]

    def step(x, gain_a, wq, wk, wv, wo, gain_m, w_gate, w_up, w_down):
        tokens, d = x.shape[1:]
        core = lax.rem(lax.axis_index("tp"), 2)
        pos = [jnp.stack([core, jnp.int32(s), jnp.int32(s == 3)]) for s in range(4)]
        angle = jnp.arange(tokens, dtype=jnp.float32)[:, None] * THETA ** (-jnp.arange(HEAD // 2, dtype=jnp.float32) / (HEAD // 2))
        cos, sin = jnp.cos(angle), jnp.sin(angle)
        cos, sin = jnp.concatenate([cos, cos], -1), jnp.concatenate([-sin, sin], -1)
        gain_a, gain_m = gain_a.reshape(1, d), gain_m.reshape(1, d)
        token, y = jnp.zeros((8, 128), jnp.float32), None

        def run(f, *args, **more):
            nonlocal token
            out, token = f(token, *args, **more)
            return out

        def send(pairs, array):
            return lax.ppermute(array, "tp", pairs)

        def attention(s, count=1):
            out, keep = run(attention_half, pos[s], x, gain_a, cos, sin, wk, wv, wq, wo, count)
            return send(core_pairs, out), keep

        def gated(s, given, pieces, **more):
            out = run(mlp, pos[s], given, w_down, pieces, **more)
            return (send(core_pairs, out[0]), *out[1:])

        def chip_sum(s, came, keep):
            term = run(add, pos[s], (keep,), (came,))
            return term, send(chip_pairs, term)

        def finish(s, base, term, came):
            own = run(add, pos[s], base, (term,), (came,))
            return own, send(core_pairs, own)

        weights = gain_m, w_gate, w_up
        a0 = attention(0)
        a1 = attention(1)
        a0 = chip_sum(0, *a0)
        a2 = attention(2, 2)
        a1 = chip_sum(1, *a1)
        h0 = finish(0, (x,), *a0)
        a2 = chip_sum(2, *a2)
        m0 = gated(0, (*h0, *weights), (0, 1))
        h1 = finish(1, (x,), *a1)
        m0 = chip_sum(0, *m0)
        m1 = gated(1, (*h1, *weights), (0, 1))
        h2 = finish(2, (x,), *a2)
        m1 = chip_sum(1, *m1)
        m2 = gated(2, (*h2, *weights), (0, 1))
        r0 = finish(0, (h0[0],), *m0)
        m2 = chip_sum(2, *m2)
        r1 = finish(1, (h1[0],), *m1)
        y = run(place, pos[0], *r0, None, x.shape)
        y = run(place, pos[1], *r1, y, x.shape)
        *m3, hidden = gated(3, (*h2, *weights), (0,), hidden_out=True)
        r2 = finish(2, (h2[0],), *m2)
        m3 = chip_sum(3, *m3)
        m4 = gated(3, (hidden,), (1,))
        y = run(place, pos[2], *r2, y, x.shape)
        m4 = chip_sum(3, *m4)
        r3 = finish(3, (h2[0], tokens, 0), *m3)
        y = run(place, pos[3], *r3, y, x.shape, 0)
        r4 = finish(3, (h2[0], tokens, PIECE), *m4)
        return run(place, pos[3], *r4, y, x.shape, 1)

    tokens, whole, columns, rows_of = P("dp", None, None), P(None), P(None, "tp"), P("tp", None)
    return jax.shard_map(
        step,
        mesh=mesh,
        in_specs=(tokens, whole, columns, columns, columns, rows_of, whole, columns, columns, rows_of),
        out_specs=tokens,
        check_vma=False,
    )
```

```python
import functools

import jax
import jax.numpy as jnp
from jax import lax
from jax.experimental import pallas as pl
from jax.experimental.pallas import tpu as pltpu
from jax.sharding import PartitionSpec as P


HEAD = 128
THETA = 10000
LOG2E = 1.4426950408889634
EPS = 1e-6
VMEM = 66_500_000
PANEL = 256
PIECE = 1280
WIDE = 768
COLS = 512

ANY = pl.BlockSpec(memory_space=pl.ANY)


def _call(kernel, token, given, grid, in_specs, out_specs, out_shape, scratch=(), aliases=None, cost=None):
    n, m = len(in_specs), len(out_specs)

    def body(*refs):
        kernel(*refs[: 1 + n], *refs[2 + n : 2 + n + m], *refs[3 + n + m :])

    out = pl.pallas_call(
        body,
        grid_spec=pltpu.PrefetchScalarGridSpec(num_scalar_prefetch=1, grid=grid, in_specs=[*in_specs, ANY], out_specs=[*out_specs, ANY],
                                               scratch_shapes=list(scratch)),
        out_shape=[*out_shape, jax.ShapeDtypeStruct((8, 128), jnp.float32)],
        input_output_aliases=aliases or {},
        compiler_params=pltpu.CompilerParams(dimension_semantics=("arbitrary",) * len(grid), vmem_limit_bytes=VMEM),
        cost_estimate=cost,
    )(*given, token)
    return out[:-1], out[-1]


def _dot(a, b, ca=1, cb=0):
    return lax.dot_general(a, b, (((ca,), (cb,)), ((), ())), preferred_element_type=jnp.float32)


def _once(shape, index_map):
    return pl.BlockSpec(shape, index_map, pipeline_mode=pl.Buffered(1))


def _norm(x_ref, gain_ref, o_ref, column, rows=64):
    tokens, d = o_ref.shape

    def some(r, _):
        at = pl.ds(pl.multiple_of(r * rows, rows), rows)
        total = jnp.zeros((rows, 128), jnp.float32)
        for c in range(d // 128):
            wide = x_ref[at, c * 128 : (c + 1) * 128].astype(jnp.float32)
            total += wide * wide
        scale = lax.rsqrt(jnp.sum(total, -1, keepdims=True) * (1 / d) + EPS)
        for c in range(d // 128):
            to = pl.ds(pl.multiple_of(column(c), 128), 128)
            wide = x_ref[at, c * 128 : (c + 1) * 128].astype(jnp.float32)
            o_ref[at, to] = (wide * scale * gain_ref[:, to].astype(jnp.float32)).astype(jnp.bfloat16)
        return _

    lax.fori_loop(0, tokens // rows, some, None)


def _rotate(t, cos, sin):
    t = t.astype(jnp.float32)
    return (t * cos + pltpu.roll(t, HEAD // 2, 1) * sin).astype(jnp.bfloat16)


def _one_head(q, k, vt, o_ref, at, tokens):
    e = HEAD**-0.5 * LOG2E
    half = tokens // 2
    for i in range(2):
        n = half * (i + 1)
        s = _dot(k[:n], q[half * i : n], 1, 1)
        key = lax.broadcasted_iota(jnp.int32, (half, half), 0)
        query = lax.broadcasted_iota(jnp.int32, (half, half), 1)
        last = jnp.where(query >= key, s[n - half :], -1e30)
        s = jnp.concatenate([s[:half], last], 0) if i else last
        top = s.max(axis=0, keepdims=True)
        p = jnp.exp2((s - top) * e).astype(jnp.bfloat16)
        mix = _dot(vt[:, :n], p)
        o = mix[:HEAD] * (1 / mix[HEAD : HEAD + 1])
        o_ref[half * i : n, pl.ds(at, HEAD)] = o.T.astype(jnp.bfloat16)


def _attention_kernel(core_ref, x_hbm, gain_ref, cos_ref, sin_ref, wk_hbm, wv_hbm, wq_hbm, wo_hbm, send_ref, keep_ref,
                      x_s, a_s, q_s, k_s, vt_s, seen_s, wk_s, wv_s, wq_s, wo_s, x_sem, w_sem, *, first, group):
    i = pl.program_id(0)
    tokens, d = a_s.shape
    kvs, nq, no = k_s.shape[0], wq_s.shape[1] // PANEL, wo_s.shape[0]
    per = no // 2

    def fetch(n):
        return pltpu.make_async_copy(x_hbm.at[first + n], x_s, x_sem)

    def copy(n, src, dst):
        return pltpu.make_async_copy(src, dst, w_sem.at[n])

    some = [pl.ds(0, 2 * PANEL), pl.ds(2 * PANEL, (nq - 2) * PANEL)]
    weights = [copy(0, wk_hbm, wk_s), copy(1, wv_hbm, wv_s)] + [copy(2 + n, wq_hbm.at[:, at], wq_s.at[:, at]) for n, at in enumerate(some)]
    for n in range(no):
        half = (1 - core_ref[0]) if n < per else core_ref[0]
        weights.append(copy(4 + n, wo_hbm.at[:, pl.ds(pl.multiple_of((half * per + n % per) * PIECE, PIECE), PIECE)], wo_s.at[n]))

    def ready(n):
        @pl.when(i == 0)
        def _():
            weights[n].wait()

    @pl.when(i == 0)
    def _():
        fetch(0).start()
        for w in weights:
            w.start()

    fetch(i).wait()
    _norm(x_s, gain_ref, a_s, lambda c: c * 128)

    @pl.when(i + 1 < pl.num_programs(0))
    def _():
        fetch(i + 1).start()

    def project(r):
        t = _dot(a_s[...], wq_s[:, pl.ds(pl.multiple_of(r * PANEL, PANEL), PANEL)]).astype(jnp.bfloat16)
        for n in range(2):
            q_s[lax.rem(r, 2), n] = _rotate(t[:, n * HEAD : (n + 1) * HEAD], cos_ref[...], sin_ref[...])

    def attend(r):
        for n in range(2):
            head = 2 * r + n
            kv = lax.div(head, group)
            _one_head(q_s[lax.rem(r, 2), n], k_s[kv], vt_s[kv], seen_s, pl.multiple_of(head * HEAD, HEAD), tokens)

    for n in range(3):
        ready(n)
    t = _dot(a_s[...], wk_s[...]).astype(jnp.bfloat16)
    for n in range(kvs):
        k_s[n] = _rotate(t[:, n * HEAD : (n + 1) * HEAD], cos_ref[...], sin_ref[...])
    t = _dot(a_s[...], wv_s[...])
    for n in range(kvs):
        vt_s[n, :HEAD, :] = t[:, n * HEAD : (n + 1) * HEAD].T.astype(jnp.bfloat16)
        vt_s[n, HEAD:, :] = jnp.ones((16, tokens), jnp.bfloat16)
    project(jnp.int32(0))
    ready(3)

    def both(r, _):
        attend(r)
        project(r + 1)
        return _

    lax.fori_loop(0, nq - 1, both, None)
    attend(jnp.int32(nq - 1))
    for n in range(no):
        ready(4 + n)
    for n in range(no):
        o_ref = send_ref if n < per else keep_ref
        o_ref[:, n % per * PIECE : (n % per + 1) * PIECE] = _dot(seen_s[...], wo_s[n]).astype(jnp.bfloat16)


def attention_half(token, core, x, gain, cos, sin, wk, wv, wq, wo, first, count):
    _, tokens, d = x.shape
    qd, kvd, half = wq.shape[1], wk.shape[1], d // 2
    no = d // PIECE
    whole = lambda i, core: (0, 0)
    out = jax.ShapeDtypeStruct((count * tokens, half), jnp.bfloat16)
    rows = pl.BlockSpec((tokens, half), lambda i, core: (i, 0))
    return _call(
        functools.partial(_attention_kernel, first=first, group=qd // kvd), token, (core, x, gain, cos, sin, wk, wv, wq, wo), (count,),
        in_specs=[ANY, _once((1, d), whole), _once((tokens, HEAD), whole), _once((tokens, HEAD), whole), ANY, ANY, ANY, ANY],
        out_specs=[rows, rows],
        out_shape=[out, out],
        scratch=[
            pltpu.VMEM((tokens, d), jnp.bfloat16),
            pltpu.VMEM((tokens, d), jnp.bfloat16),
            pltpu.VMEM((2, 2, tokens, HEAD), jnp.bfloat16),
            pltpu.VMEM((kvd // HEAD, tokens, HEAD), jnp.bfloat16),
            pltpu.VMEM((kvd // HEAD, HEAD + 16, tokens), jnp.bfloat16),
            pltpu.VMEM((tokens, qd), jnp.bfloat16),
            pltpu.VMEM((d, kvd), jnp.bfloat16),
            pltpu.VMEM((d, kvd), jnp.bfloat16),
            pltpu.VMEM((d, qd), jnp.bfloat16),
            pltpu.VMEM((no, qd, PIECE), jnp.bfloat16),
            pltpu.SemaphoreType.DMA,
            pltpu.SemaphoreType.DMA((4 + no,)),
        ],
        cost=pl.CostEstimate(
            flops=count * (2 * tokens * d * (2 * qd + 2 * kvd) + 4 * tokens * tokens * qd),
            transcendentals=count * tokens * tokens * qd // HEAD,
            bytes_accessed=2 * (2 * count * tokens * d + d * (2 * qd + 2 * kvd))),
    )


def _mlp_kernel(core_ref, *refs, nf, pieces, row, hidden_in, hidden_out):
    if hidden_in:
        hid_hbm, wd_hbm, send_hbm, keep_hbm, w_s, hid_s, t_s, w_sem, h_sem, t_sem = refs
    elif hidden_out:
        own_hbm, sib_hbm, gain_ref, wg_hbm, wu_hbm, wd_hbm, send_hbm, keep_hbm, hid_hbm, w_s, b_s, hid_s, t_s, w_sem, h_sem, t_sem = refs
    else:
        own_hbm, sib_hbm, gain_ref, wg_hbm, wu_hbm, wd_hbm, send_hbm, keep_hbm, w_s, b_s, hid_s, t_s, w_sem, h_sem, t_sem = refs
    j = pl.program_id(0)
    tokens, ff = hid_s.shape
    half = wd_hbm.shape[1] // 2
    per, last = len(pieces), nf + len(pieces)

    def slot(i, step):
        return 2 * lax.rem(step, 2) + i

    def gate_up(i, step):
        src, at = (wg_hbm, wu_hbm)[i], slot(i, step)
        column = pl.multiple_of(step * WIDE, WIDE)
        return pltpu.make_async_copy(src.at[:, pl.ds(column, WIDE)], w_s.at[at, pl.ds(0, src.shape[0]), :], w_sem.at[at])

    def down(i, step):
        q, at = 2 * (step - nf) + i, slot(i, step)
        core = jnp.where(q < per, 1 - core_ref[0], core_ref[0])
        column = pl.multiple_of(core * half + (lax.rem(q, per) + pieces[0]) * COLS, COLS)
        return pltpu.make_async_copy(wd_hbm.at[:, pl.ds(column, COLS)], w_s.at[at, :, pl.ds(0, COLS)], w_sem.at[at])

    def start(step):
        if nf:
            @pl.when(step < nf)
            def _():
                for i in range(2):
                    gate_up(i, step).start()

        @pl.when((step >= nf) & (step < last))
        def _():
            for i in range(2):
                down(i, step).start()

    def out(q, begin):
        to, at = pl.multiple_of(lax.rem(q, per) * COLS, COLS), lax.rem(q, 4)
        for ref, now in ((send_hbm, q < per), (keep_hbm, q >= per)):
            @pl.when(now)
            def _():
                copy = pltpu.make_async_copy(t_s.at[at], ref.at[:, pl.ds(to, COLS)], t_sem.at[at])
                copy.start() if begin else copy.wait()

    if hidden_in:
        first = [pltpu.make_async_copy(hid_hbm, hid_s, h_sem.at[0])]
    else:
        first = [pltpu.make_async_copy(ref.at[pl.ds(row, tokens)], hid_s.at[:, pl.ds(n * half, half)], h_sem.at[n])
                 for n, ref in enumerate((own_hbm, sib_hbm))]

    @pl.when(j == 0)
    def _():
        for copy in first:
            copy.start()
        start(jnp.int32(0))

    start(j + 1)

    @pl.when(j == 0)
    def _():
        for copy in first:
            copy.wait()
        if not hidden_in:
            shift = core_ref[0] * half
            _norm(hid_s, gain_ref, b_s, lambda c: lax.rem(shift + c * 128, 2 * half))

    if nf:
        @pl.when(j < nf)
        def _():
            for i in range(2):
                gate_up(i, j).wait()
            d = b_s.shape[1]
            for p in range(WIDE // PANEL):
                at = slice(p * PANEL, (p + 1) * PANEL)
                gate = _dot(b_s[...], w_s[slot(0, j), :d, at])
                up = _dot(b_s[...], w_s[slot(1, j), :d, at])
                to = pl.ds(pl.multiple_of(j * WIDE + p * PANEL, PANEL), PANEL)
                hid_s[:, to] = (gate * jax.nn.sigmoid(gate) * up).astype(jnp.bfloat16)

    if hidden_out:
        put = pltpu.make_async_copy(hid_s, hid_hbm, h_sem.at[0])

        @pl.when(j == nf)
        def _():
            put.start()

    @pl.when(j >= nf)
    def _():
        q = 2 * (j - nf)

        @pl.when(q >= 4)
        def _():
            for i in range(2):
                out(q - 4 + i, False)

        for i in range(2):
            down(i, j).wait()
        for i in range(2):
            t_s[lax.rem(q + i, 4)] = _dot(hid_s[...], w_s[slot(i, j), :, :COLS]).astype(jnp.bfloat16)
        for i in range(2):
            out(q + i, True)

        @pl.when(j == last - 1)
        def _():
            for i in range(-2, 2):
                out(q + i, False)
            if hidden_out:
                put.wait()


def mlp(token, core, given, wd, pieces, row=0, hidden_out=False):
    ff, d = wd.shape
    tokens, hidden_in = 512, len(given) == 1
    per = len(pieces)
    nf = 0 if hidden_in else ff // WIDE
    out = jax.ShapeDtypeStruct((tokens, per * COLS), jnp.bfloat16)
    hidden = jax.ShapeDtypeStruct((tokens, ff), jnp.bfloat16)
    flops = (0 if hidden_in else 4 * tokens * d * ff) + 2 * tokens * ff * 2 * per * COLS
    return _call(
        functools.partial(_mlp_kernel, nf=nf, pieces=pieces, row=row, hidden_in=hidden_in, hidden_out=hidden_out), token, (core, *given, wd),
        (nf + per,),
        in_specs=[ANY, ANY] if hidden_in else [ANY, ANY, _once((1, d), lambda j, core: (0, 0)), ANY, ANY, ANY],
        out_specs=[ANY] * (2 + hidden_out),
        out_shape=[out, out] + [hidden] * hidden_out,
        scratch=[pltpu.VMEM((4, ff, COLS if hidden_in else WIDE), jnp.bfloat16)]
        + [pltpu.VMEM((tokens, d), jnp.bfloat16)] * (not hidden_in)
        + [
            pltpu.VMEM((tokens, ff), jnp.bfloat16),
            pltpu.VMEM((4, tokens, COLS), jnp.bfloat16),
            pltpu.SemaphoreType.DMA((4,)),
            pltpu.SemaphoreType.DMA((2,)),
            pltpu.SemaphoreType.DMA((4,)),
        ],
        cost=pl.CostEstimate(flops=flops, transcendentals=tokens * ff, bytes_accessed=flops // tokens + 4 * tokens * d),
    )


def _sums_kernel(core_ref, *refs, jobs, count, fresh, aliased):
    arrays, refs = refs[:count], refs[count:]
    made, refs = refs[: fresh], refs[fresh:]
    y_hbm, refs = (refs[0], refs[1:]) if aliased else (None, refs)
    core = core_ref[0]
    rows = 128
    todo = []
    at_array = at_made = 0
    for seq, terms, keep, to, size, wide in jobs:
        sem, osem, o_s, *t_s = refs[: 3 + len(terms)]
        refs = refs[3 + len(terms) :]
        held = arrays[at_array : at_array + len(terms)]
        at_array += len(terms)
        out = made[at_made] if keep else None
        at_made += bool(keep)
        for r in range(size // rows):
            here = pl.ds(r * rows, rows)
            ins, outs = [], []
            for n, ((row, column), array) in enumerate(zip(terms, held)):
                if len(array.shape) == 3:
                    half = array.shape[2] // 2
                    src = array.at[seq + r * rows // 512, pl.ds(r * rows % 512, rows), pl.ds(pl.multiple_of(core * half, 128), wide)]
                else:
                    src = array.at[pl.ds(row + r * rows, rows), pl.ds(column, wide)]
                ins.append(pltpu.make_async_copy(src, t_s[n].at[here], sem.at[n, r]))
            from_s = o_s if len(terms) > 1 else t_s[0]
            if keep:
                outs.append(pltpu.make_async_copy(from_s.at[here], out.at[here], osem.at[0, r]))
            if to is not None:
                mine, column = to
                half = y_hbm.shape[2] // 2
                start = pl.multiple_of((core if mine else 1 - core) * half + column, 128)
                outs.append(pltpu.make_async_copy(from_s.at[here], y_hbm.at[seq, here, pl.ds(start, wide)], osem.at[1, r]))

            def work(o_s=o_s, t_s=t_s, first=r * rows, rows=rows):
                def some(k, _):
                    at = pl.ds(pl.multiple_of(first + k * 16, 16), 16)
                    total = None
                    for t in t_s[::-1]:
                        t = t[at, :].astype(jnp.float32)
                        total = t if total is None else t + total
                    o_s[at, :] = total.astype(jnp.bfloat16)
                    return _

                if len(t_s) > 1:
                    lax.fori_loop(0, rows // 16, some, None)

            todo.append((ins, outs, work))
    for ins, _, _ in todo:
        for copy in ins:
            copy.start()
    for ins, outs, work in todo:
        for copy in ins:
            copy.wait()
        work()
        for copy in outs:
            copy.start()
    for _, outs, _ in todo:
        for copy in outs:
            copy.wait()


def sums(token, core, jobs, y=None, shape=None):
    given, plain, scratch, out_shape, work = [], [], [], [], 0
    for seq, terms, keep, to in jobs:
        terms = [(t + (0, 0))[:3] for t in terms]
        size, wide = terms[-1][0].shape
        given += [t[0] for t in terms]
        plain.append((seq, [t[1:] for t in terms], keep, to, size, wide))
        buffer = pltpu.VMEM((size, wide), jnp.bfloat16)
        scratch += [pltpu.SemaphoreType.DMA((len(terms), size // 128)), pltpu.SemaphoreType.DMA((2, size // 128))]
        scratch += [buffer if len(terms) > 1 else pltpu.VMEM((16, 128), jnp.bfloat16)] + [buffer] * len(terms)
        out_shape += [jax.ShapeDtypeStruct((size, wide), jnp.bfloat16)] * bool(keep)
        work += (len(terms) + 1) * size * wide
    count, fresh = len(given), len(out_shape)
    aliased = any(to is not None for *_, to in jobs)
    if aliased:
        out_shape.append(jax.ShapeDtypeStruct(shape, jnp.bfloat16))
    had = aliased and y is not None

    def kernel(core_ref, *refs):
        _sums_kernel(core_ref, *refs[:count], *refs[count + had :], jobs=plain, count=count, fresh=fresh, aliased=aliased)

    out, token = _call(
        kernel, token, (core, *given, *([y] if had else [])), (1,),
        in_specs=[ANY] * (count + had),
        out_specs=[ANY] * len(out_shape),
        out_shape=out_shape,
        scratch=scratch,
        aliases={1 + count: fresh} if had else None,
        cost=pl.CostEstimate(flops=work, transcendentals=0, bytes_accessed=2 * work),
    )
    return tuple(out), token


def solution(mesh):
    n = mesh.shape["tp"]
    core_pairs = [(i, i ^ 1) for i in range(n)]
    chip_pairs = [(i, i ^ 2) for i in range(n)]

    def step(x, gain_a, wq, wk, wv, wo, gain_m, w_gate, w_up, w_down):
        tokens, d = x.shape[1:]
        core = lax.rem(lax.axis_index("tp"), 2).reshape(1)
        angle = jnp.arange(tokens, dtype=jnp.float32)[:, None] * THETA ** (-jnp.arange(HEAD // 2, dtype=jnp.float32) / (HEAD // 2))
        cos, sin = jnp.cos(angle), jnp.sin(angle)
        cos, sin = jnp.concatenate([cos, cos], -1), jnp.concatenate([-sin, sin], -1)
        gain_a, gain_m = gain_a.reshape(1, d), gain_m.reshape(1, d)
        token, y = jnp.zeros((8, 128), jnp.float32), None

        def run(f, *args, **more):
            nonlocal token
            out, token = f(token, core, *args, **more)
            return out

        def send(pairs, array):
            return lax.ppermute(array, "tp", pairs)

        def attention(s, count=1):
            out, keep = run(attention_half, x, gain_a, cos, sin, wk, wv, wq, wo, s, count)
            return send(core_pairs, out), keep

        def gated(given, pieces, **more):
            out = run(mlp, given, w_down, pieces, **more)
            return (send(core_pairs, out[0]), *out[1:])

        def chip_sum(came, keep):
            (term,) = run(sums, [(0, [(keep,), (came,)], True, None)])
            return term, send(chip_pairs, term)

        def residual(s, term, came):
            (own,) = run(sums, [(s, [(x,), (term,), (came,)], True, None)])
            return own, send(core_pairs, own)

        def finish(s, base, column, term, came, others=()):
            nonlocal y
            mine = (s, [base, (term,), (came,)], True, (True, column))
            own, y = run(sums, [mine, *others], y, x.shape)
            return send(core_pairs, own)

        def put(s, came, column=0):
            return s, [(came,)], False, (False, column)

        weights = gain_m, w_gate, w_up
        every = tuple(range(d // 2 // COLS))
        cut = 3
        a0 = attention(0)
        a1 = attention(1)
        a0 = chip_sum(*a0)
        a2 = attention(2, 2)
        a1 = chip_sum(*a1)
        h0 = residual(0, *a0)
        a2 = chip_sum(*a2)
        m0 = gated((*h0, *weights), every)
        h1 = residual(1, *a1)
        m0 = chip_sum(*m0)
        m1 = gated((*h1, *weights), every)
        h2 = residual(2, *a2)
        m1 = chip_sum(*m1)
        m2 = gated((*h2, *weights), every)
        r0 = finish(0, (h0[0],), 0, *m0)
        m2 = chip_sum(*m2)
        r1 = finish(1, (h1[0],), 0, *m1, [put(0, r0)])
        *m3, hidden = gated((*h2, *weights), every[:cut], row=tokens, hidden_out=True)
        r2 = finish(2, (h2[0],), 0, *m2, [put(1, r1)])
        m3 = chip_sum(*m3)
        m4 = gated((hidden,), every[cut:])
        y = run(sums, [put(2, r2)], y, x.shape)[0]
        m4 = chip_sum(*m4)
        r3 = finish(3, (h2[0], tokens, 0), 0, *m3)
        y = run(sums, [put(3, r3)], y, x.shape)[0]
        r4 = finish(3, (h2[0], tokens, cut * COLS), cut * COLS, *m4)
        return run(sums, [put(3, r4, cut * COLS)], y, x.shape)[0]

    tokens, whole, columns, rows_of = P("dp", None, None), P(None), P(None, "tp"), P("tp", None)
    return jax.shard_map(
        step,
        mesh=mesh,
        in_specs=(tokens, whole, columns, columns, columns, rows_of, whole, columns, columns, rows_of),
        out_specs=tokens,
        check_vma=False,
    )
```

```python
import functools

import jax
import jax.numpy as jnp
from jax import lax
from jax.experimental import pallas as pl
from jax.experimental.pallas import tpu as pltpu
from jax.sharding import PartitionSpec as P


HEAD = 128
THETA = 10000
LOG2E = 1.4426950408889634
EPS = 1e-6
VMEM = 66_500_000
PANEL = 256
PIECE = 1280
WIDE = 768
COLS = 512

ANY = pl.BlockSpec(memory_space=pl.ANY)


def _call(kernel, token, given, grid, in_specs, out_specs, out_shape, scratch=(), aliases=None, cost=None):
    n, m = len(in_specs), len(out_specs)

    def body(*refs):
        kernel(*refs[: 1 + n], *refs[2 + n : 2 + n + m], *refs[3 + n + m :])

    out = pl.pallas_call(
        body,
        grid_spec=pltpu.PrefetchScalarGridSpec(num_scalar_prefetch=1, grid=grid, in_specs=[*in_specs, ANY], out_specs=[*out_specs, ANY],
                                               scratch_shapes=list(scratch)),
        out_shape=[*out_shape, jax.ShapeDtypeStruct((8, 128), jnp.float32)],
        input_output_aliases=aliases or {},
        compiler_params=pltpu.CompilerParams(dimension_semantics=("arbitrary",) * len(grid), vmem_limit_bytes=VMEM),
        cost_estimate=cost,
    )(*given, token)
    return out[:-1], out[-1]


def _dot(a, b, ca=1, cb=0):
    return lax.dot_general(a, b, (((ca,), (cb,)), ((), ())), preferred_element_type=jnp.float32)


def _once(shape, index_map):
    return pl.BlockSpec(shape, index_map, pipeline_mode=pl.Buffered(1))


def _norm(x_ref, gain_ref, o_ref, column, rows=64):
    tokens, d = o_ref.shape

    def some(r, _):
        at = pl.ds(pl.multiple_of(r * rows, rows), rows)
        total = jnp.zeros((rows, 128), jnp.float32)
        for c in range(d // 128):
            wide = x_ref[at, c * 128 : (c + 1) * 128].astype(jnp.float32)
            total += wide * wide
        scale = lax.rsqrt(jnp.sum(total, -1, keepdims=True) * (1 / d) + EPS)
        for c in range(d // 128):
            to = pl.ds(pl.multiple_of(column(c), 128), 128)
            wide = x_ref[at, c * 128 : (c + 1) * 128].astype(jnp.float32)
            o_ref[at, to] = (wide * scale * gain_ref[:, to].astype(jnp.float32)).astype(jnp.bfloat16)
        return _

    lax.fori_loop(0, tokens // rows, some, None)


def _rotate(t, cos, sin):
    t = t.astype(jnp.float32)
    return (t * cos + pltpu.roll(t, HEAD // 2, 1) * sin).astype(jnp.bfloat16)


def _scores(q, k):
    half = q.shape[0] // 2
    return [_dot(k[: half * (i + 1)], q[half * i : half * (i + 1)], 1, 1) for i in range(2)]


def _weigh(scores, vt, o_ref, at):
    e = HEAD**-0.5 * LOG2E
    for i, s in enumerate(scores):
        n, half = s.shape
        key = lax.broadcasted_iota(jnp.int32, (half, half), 0)
        query = lax.broadcasted_iota(jnp.int32, (half, half), 1)
        last = jnp.where(query >= key, s[n - half :], -1e30)
        s = jnp.concatenate([s[: n - half], last], 0) if i else last
        top = s.max(axis=0, keepdims=True)
        p = jnp.exp2((s - top) * e).astype(jnp.bfloat16)
        mix = _dot(vt[:, :n], p)
        o = mix[:HEAD] * (1 / mix[HEAD : HEAD + 1])
        o_ref[n - half : n, pl.ds(at, HEAD)] = o.T.astype(jnp.bfloat16)


def _attention_kernel(core_ref, x_hbm, gain_ref, cos_ref, sin_ref, wk_hbm, wv_hbm, wq_hbm, wo_hbm, send_ref, keep_ref,
                      x_s, a_s, q_s, k_s, vt_s, seen_s, wk_s, wv_s, wq_s, wo_s, x_sem, w_sem, *, first, group):
    i = pl.program_id(0)
    tokens, d = a_s.shape
    kvs, nq, no = k_s.shape[0], wq_s.shape[1] // PANEL, wo_s.shape[0]
    per = no // 2

    def fetch(n):
        return pltpu.make_async_copy(x_hbm.at[first + n], x_s, x_sem)

    def copy(n, src, dst):
        return pltpu.make_async_copy(src, dst, w_sem.at[n])

    some = [pl.ds(0, 2 * PANEL), pl.ds(2 * PANEL, (nq - 2) * PANEL)]
    weights = [copy(0, wk_hbm, wk_s), copy(1, wv_hbm, wv_s)] + [copy(2 + n, wq_hbm.at[:, at], wq_s.at[:, at]) for n, at in enumerate(some)]
    for n in range(no):
        half = (1 - core_ref[0]) if n < per else core_ref[0]
        weights.append(copy(4 + n, wo_hbm.at[:, pl.ds(pl.multiple_of((half * per + n % per) * PIECE, PIECE), PIECE)], wo_s.at[n]))

    def ready(n):
        @pl.when(i == 0)
        def _():
            weights[n].wait()

    def begin(these):
        @pl.when(i == 0)
        def _():
            for w in these:
                w.start()

    begin([fetch(0)])
    fetch(i).wait()
    begin(weights[:3])
    _norm(x_s, gain_ref, a_s, lambda c: c * 128)
    begin(weights[3:])

    @pl.when(i + 1 < pl.num_programs(0))
    def _():
        fetch(i + 1).start()

    def project(r):
        return _dot(a_s[...], wq_s[:, pl.ds(pl.multiple_of(r * PANEL, PANEL), PANEL)]).astype(jnp.bfloat16)

    def turn(t, r):
        for n in range(2):
            q_s[lax.rem(r, 2), n] = _rotate(t[:, n * HEAD : (n + 1) * HEAD], cos_ref[...], sin_ref[...])

    def attend(r, beside):
        heads = [2 * r + n for n in range(2)]
        kv = [lax.div(head, group) for head in heads]
        scores = [_scores(q_s[lax.rem(r, 2), n], k_s[kv[n]]) for n in range(2)]
        got = beside()
        for n in range(2):
            _weigh(scores[n], vt_s[kv[n]], seen_s, pl.multiple_of(heads[n] * HEAD, HEAD))
        return got

    for n in range(3):
        ready(n)
    t = _dot(a_s[...], wk_s[...]).astype(jnp.bfloat16)
    for n in range(kvs):
        k_s[n] = _rotate(t[:, n * HEAD : (n + 1) * HEAD], cos_ref[...], sin_ref[...])
    t = _dot(a_s[...], wv_s[...])
    for n in range(kvs):
        vt_s[n, :HEAD, :] = t[:, n * HEAD : (n + 1) * HEAD].T.astype(jnp.bfloat16)
        vt_s[n, HEAD:, :] = jnp.ones((16, tokens), jnp.bfloat16)
    turn(project(0), 0)
    ready(3)

    def both(r, _):
        turn(attend(r, lambda: project(r + 1)), r + 1)
        return _

    lax.fori_loop(0, nq - 1, both, None)
    attend(jnp.int32(nq - 1), lambda: None)
    for n in range(no):
        ready(4 + n)
    for n in range(no):
        o_ref = send_ref if n < per else keep_ref
        o_ref[:, n % per * PIECE : (n % per + 1) * PIECE] = _dot(seen_s[...], wo_s[n]).astype(jnp.bfloat16)


def attention_half(token, core, x, gain, cos, sin, wk, wv, wq, wo, first, count):
    _, tokens, d = x.shape
    qd, kvd, half = wq.shape[1], wk.shape[1], d // 2
    no = d // PIECE
    whole = lambda i, core: (0, 0)
    out = jax.ShapeDtypeStruct((count * tokens, half), jnp.bfloat16)
    rows = pl.BlockSpec((tokens, half), lambda i, core: (i, 0))
    return _call(
        functools.partial(_attention_kernel, first=first, group=qd // kvd), token, (core, x, gain, cos, sin, wk, wv, wq, wo), (count,),
        in_specs=[ANY, _once((1, d), whole), _once((tokens, HEAD), whole), _once((tokens, HEAD), whole), ANY, ANY, ANY, ANY],
        out_specs=[rows, rows],
        out_shape=[out, out],
        scratch=[
            pltpu.VMEM((tokens, d), jnp.bfloat16),
            pltpu.VMEM((tokens, d), jnp.bfloat16),
            pltpu.VMEM((2, 2, tokens, HEAD), jnp.bfloat16),
            pltpu.VMEM((kvd // HEAD, tokens, HEAD), jnp.bfloat16),
            pltpu.VMEM((kvd // HEAD, HEAD + 16, tokens), jnp.bfloat16),
            pltpu.VMEM((tokens, qd), jnp.bfloat16),
            pltpu.VMEM((d, kvd), jnp.bfloat16),
            pltpu.VMEM((d, kvd), jnp.bfloat16),
            pltpu.VMEM((d, qd), jnp.bfloat16),
            pltpu.VMEM((no, qd, PIECE), jnp.bfloat16),
            pltpu.SemaphoreType.DMA,
            pltpu.SemaphoreType.DMA((4 + no,)),
        ],
        cost=pl.CostEstimate(
            flops=count * (2 * tokens * d * (2 * qd + 2 * kvd) + 4 * tokens * tokens * qd),
            transcendentals=count * tokens * tokens * qd // HEAD,
            bytes_accessed=2 * (2 * count * tokens * d + d * (2 * qd + 2 * kvd))),
    )


def _mlp_kernel(core_ref, *refs, nf, pieces, row, hidden_in, hidden_out):
    if hidden_in:
        hid_hbm, wd_hbm, send_hbm, keep_hbm, w_s, hid_s, t_s, w_sem, h_sem, t_sem = refs
    elif hidden_out:
        own_hbm, sib_hbm, gain_ref, wg_hbm, wu_hbm, wd_hbm, send_hbm, keep_hbm, hid_hbm, w_s, b_s, hid_s, t_s, w_sem, h_sem, t_sem = refs
    else:
        own_hbm, sib_hbm, gain_ref, wg_hbm, wu_hbm, wd_hbm, send_hbm, keep_hbm, w_s, b_s, hid_s, t_s, w_sem, h_sem, t_sem = refs
    j = pl.program_id(0)
    tokens, ff = hid_s.shape
    half = wd_hbm.shape[1] // 2
    per, last = len(pieces), nf + len(pieces)

    def slot(i, step):
        return 2 * lax.rem(step, 2) + i

    def gate_up(i, step):
        src, at = (wg_hbm, wu_hbm)[i], slot(i, step)
        column = pl.multiple_of(step * WIDE, WIDE)
        return pltpu.make_async_copy(src.at[:, pl.ds(column, WIDE)], w_s.at[at, pl.ds(0, src.shape[0]), :], w_sem.at[at])

    def down(i, step):
        q, at = 2 * (step - nf) + i, slot(i, step)
        core = jnp.where(q < per, 1 - core_ref[0], core_ref[0])
        column = pl.multiple_of(core * half + (lax.rem(q, per) + pieces[0]) * COLS, COLS)
        return pltpu.make_async_copy(wd_hbm.at[:, pl.ds(column, COLS)], w_s.at[at, :, pl.ds(0, COLS)], w_sem.at[at])

    def start(step):
        if nf:
            @pl.when(step < nf)
            def _():
                for i in range(2):
                    gate_up(i, step).start()

        @pl.when((step >= nf) & (step < last))
        def _():
            for i in range(2):
                down(i, step).start()

    def out(q, begin):
        to, at = pl.multiple_of(lax.rem(q, per) * COLS, COLS), lax.rem(q, 4)
        for ref, now in ((send_hbm, q < per), (keep_hbm, q >= per)):
            @pl.when(now)
            def _():
                copy = pltpu.make_async_copy(t_s.at[at], ref.at[:, pl.ds(to, COLS)], t_sem.at[at])
                copy.start() if begin else copy.wait()

    if hidden_in:
        first = [pltpu.make_async_copy(hid_hbm, hid_s, h_sem.at[0])]
    else:
        first = [pltpu.make_async_copy(ref.at[pl.ds(row, tokens)], hid_s.at[:, pl.ds(n * half, half)], h_sem.at[n])
                 for n, ref in enumerate((own_hbm, sib_hbm))]

    @pl.when(j == 0)
    def _():
        for copy in first:
            copy.start()
        if hidden_in:
            down(0, j).start()
        for copy in first:
            copy.wait()
        if hidden_in:
            down(1, j).start()
        else:
            start(j)
            shift = core_ref[0] * half
            _norm(hid_s, gain_ref, b_s, lambda c: lax.rem(shift + c * 128, 2 * half))

    start(j + 1)

    if nf:
        @pl.when(j < nf)
        def _():
            for i in range(2):
                gate_up(i, j).wait()
            d = b_s.shape[1]
            for p in range(WIDE // PANEL):
                at = slice(p * PANEL, (p + 1) * PANEL)
                gate = _dot(b_s[...], w_s[slot(0, j), :d, at])
                up = _dot(b_s[...], w_s[slot(1, j), :d, at])
                to = pl.ds(pl.multiple_of(j * WIDE + p * PANEL, PANEL), PANEL)
                hid_s[:, to] = (gate * jax.nn.sigmoid(gate) * up).astype(jnp.bfloat16)

    if hidden_out:
        put = pltpu.make_async_copy(hid_s, hid_hbm, h_sem.at[0])

        @pl.when(j == nf)
        def _():
            put.start()

    @pl.when(j >= nf)
    def _():
        q = 2 * (j - nf)

        @pl.when(q >= 4)
        def _():
            for i in range(2):
                out(q - 4 + i, False)

        if not hidden_in:
            for i in range(2):
                down(i, j).wait()
        for i in range(2):
            if hidden_in:
                down(i, j).wait()
            t_s[lax.rem(q + i, 4)] = _dot(hid_s[...], w_s[slot(i, j), :, :COLS]).astype(jnp.bfloat16)
        for i in range(2):
            out(q + i, True)

        @pl.when(j == last - 1)
        def _():
            for i in range(-2, 2):
                out(q + i, False)
            if hidden_out:
                put.wait()


def mlp(token, core, given, wd, pieces, row=0, hidden_out=False):
    ff, d = wd.shape
    tokens, hidden_in = 512, len(given) == 1
    per = len(pieces)
    nf = 0 if hidden_in else ff // WIDE
    out = jax.ShapeDtypeStruct((tokens, per * COLS), jnp.bfloat16)
    hidden = jax.ShapeDtypeStruct((tokens, ff), jnp.bfloat16)
    flops = (0 if hidden_in else 4 * tokens * d * ff) + 2 * tokens * ff * 2 * per * COLS
    return _call(
        functools.partial(_mlp_kernel, nf=nf, pieces=pieces, row=row, hidden_in=hidden_in, hidden_out=hidden_out), token, (core, *given, wd),
        (nf + per,),
        in_specs=[ANY, ANY] if hidden_in else [ANY, ANY, _once((1, d), lambda j, core: (0, 0)), ANY, ANY, ANY],
        out_specs=[ANY] * (2 + hidden_out),
        out_shape=[out, out] + [hidden] * hidden_out,
        scratch=[pltpu.VMEM((4, ff, COLS if hidden_in else WIDE), jnp.bfloat16)]
        + [pltpu.VMEM((tokens, d), jnp.bfloat16)] * (not hidden_in)
        + [
            pltpu.VMEM((tokens, ff), jnp.bfloat16),
            pltpu.VMEM((4, tokens, COLS), jnp.bfloat16),
            pltpu.SemaphoreType.DMA((4,)),
            pltpu.SemaphoreType.DMA((2,)),
            pltpu.SemaphoreType.DMA((4,)),
        ],
        cost=pl.CostEstimate(flops=flops, transcendentals=tokens * ff, bytes_accessed=flops // tokens + 4 * tokens * d),
    )


def _sums_kernel(core_ref, *refs, jobs, count, fresh, aliased):
    arrays, refs = refs[:count], refs[count:]
    made, refs = refs[: fresh], refs[fresh:]
    y_hbm, refs = (refs[0], refs[1:]) if aliased else (None, refs)
    core = core_ref[0]
    rows = 128
    todo = []
    at_array = at_made = 0
    for seq, terms, keep, to, size, wide in jobs:
        sem, osem, o_s, *t_s = refs[: 3 + len(terms)]
        refs = refs[3 + len(terms) :]
        held = arrays[at_array : at_array + len(terms)]
        at_array += len(terms)
        out = made[at_made] if keep else None
        at_made += bool(keep)
        for r in range(size // rows):
            here = pl.ds(r * rows, rows)
            ins, outs = [], []
            for n, ((row, column), array) in enumerate(zip(terms, held)):
                if len(array.shape) == 3:
                    half = array.shape[2] // 2
                    src = array.at[seq + r * rows // 512, pl.ds(r * rows % 512, rows), pl.ds(pl.multiple_of(core * half, 128), wide)]
                else:
                    src = array.at[pl.ds(row + r * rows, rows), pl.ds(column, wide)]
                ins.append(pltpu.make_async_copy(src, t_s[n].at[here], sem.at[n, r]))
            from_s = o_s if len(terms) > 1 else t_s[0]
            if keep:
                outs.append(pltpu.make_async_copy(from_s.at[here], out.at[here], osem.at[0, r]))
            if to is not None:
                mine, column = to
                half = y_hbm.shape[2] // 2
                start = pl.multiple_of((core if mine else 1 - core) * half + column, 128)
                outs.append(pltpu.make_async_copy(from_s.at[here], y_hbm.at[seq, here, pl.ds(start, wide)], osem.at[1, r]))

            def work(o_s=o_s, t_s=t_s, first=r * rows, rows=rows):
                def some(k, _):
                    at = pl.ds(pl.multiple_of(first + k * 16, 16), 16)
                    total = None
                    for t in t_s[::-1]:
                        t = t[at, :].astype(jnp.float32)
                        total = t if total is None else t + total
                    o_s[at, :] = total.astype(jnp.bfloat16)
                    return _

                if len(t_s) > 1:
                    lax.fori_loop(0, rows // 16, some, None)

            todo.append((ins, outs, work))
    for ins, _, _ in todo:
        for copy in ins:
            copy.start()
    for ins, outs, work in todo:
        for copy in ins:
            copy.wait()
        work()
        for copy in outs:
            copy.start()
    for _, outs, _ in todo:
        for copy in outs:
            copy.wait()


def sums(token, core, jobs, y=None, shape=None, whole=False):
    given, plain, scratch, out_shape, work = [], [], [], [], 0
    for seq, terms, keep, to in jobs:
        terms = [(t + (0, 0))[:3] for t in terms]
        size, wide = terms[-1][0].shape
        size = size if whole else min(size, 512)
        given += [t[0] for t in terms]
        plain.append((seq, [t[1:] for t in terms], keep, to, size, wide))
        buffer = pltpu.VMEM((size, wide), jnp.bfloat16)
        scratch += [pltpu.SemaphoreType.DMA((len(terms), size // 128)), pltpu.SemaphoreType.DMA((2, size // 128))]
        scratch += [buffer if len(terms) > 1 else pltpu.VMEM((16, 128), jnp.bfloat16)] + [buffer] * len(terms)
        out_shape += [jax.ShapeDtypeStruct((size, wide), jnp.bfloat16)] * bool(keep)
        work += (len(terms) + 1) * size * wide
    count, fresh = len(given), len(out_shape)
    aliased = any(to is not None for *_, to in jobs)
    if aliased:
        out_shape.append(jax.ShapeDtypeStruct(shape, jnp.bfloat16))
    had = aliased and y is not None

    def kernel(core_ref, *refs):
        _sums_kernel(core_ref, *refs[:count], *refs[count + had :], jobs=plain, count=count, fresh=fresh, aliased=aliased)

    out, token = _call(
        kernel, token, (core, *given, *([y] if had else [])), (1,),
        in_specs=[ANY] * (count + had),
        out_specs=[ANY] * len(out_shape),
        out_shape=out_shape,
        scratch=scratch,
        aliases={1 + count: fresh} if had else None,
        cost=pl.CostEstimate(flops=work, transcendentals=0, bytes_accessed=2 * work),
    )
    return tuple(out), token


def solution(mesh):
    n = mesh.shape["tp"]
    core_pairs = [(i, i ^ 1) for i in range(n)]
    chip_pairs = [(i, i ^ 2) for i in range(n)]

    def step(x, gain_a, wq, wk, wv, wo, gain_m, w_gate, w_up, w_down):
        tokens, d = x.shape[1:]
        core = lax.rem(lax.axis_index("tp"), 2).reshape(1)
        angle = jnp.arange(tokens, dtype=jnp.float32)[:, None] * THETA ** (-jnp.arange(HEAD // 2, dtype=jnp.float32) / (HEAD // 2))
        cos, sin = jnp.cos(angle), jnp.sin(angle)
        cos, sin = jnp.concatenate([cos, cos], -1), jnp.concatenate([-sin, sin], -1)
        gain_a, gain_m = gain_a.reshape(1, d), gain_m.reshape(1, d)
        token, y = cos, None

        def run(f, *args, **more):
            nonlocal token
            out, token = f(token, core, *args, **more)
            return out

        def send(pairs, array):
            return lax.ppermute(array, "tp", pairs)

        def attention(s, count=1):
            out, keep = run(attention_half, x, gain_a, cos, sin, wk, wv, wq, wo, s, count)
            return send(core_pairs, out), keep

        def gated(given, pieces, **more):
            out = run(mlp, given, w_down, pieces, **more)
            return (send(core_pairs, out[0]), *out[1:])

        def chip_sum(came, keep):
            (term,) = run(sums, [(0, [(keep,), (came,)], True, None)], whole=True)
            return term, send(chip_pairs, term)

        def residual(s, term, came, row=0):
            (own,) = run(sums, [(s, [(x,), (term, row), (came, row)], True, None)])
            return own, send(core_pairs, own)

        def finish(s, base, column, term, came, others=()):
            nonlocal y
            mine = (s, [base, (term,), (came,)], True, (True, column))
            own, y = run(sums, [mine, *others], y, x.shape)
            return send(core_pairs, own)

        def put(s, came, column=0):
            return s, [(came,)], False, (False, column)

        weights = gain_m, w_gate, w_up
        every = tuple(range(d // 2 // COLS))
        cut = 3
        a0 = attention(0)
        a1 = attention(1)
        a0 = chip_sum(*a0)
        a2 = attention(2, 2)
        a1 = chip_sum(*a1)
        h0 = residual(0, *a0)
        a2 = chip_sum(*a2)
        m0 = gated((*h0, *weights), every)
        h1 = residual(1, *a1)
        m0 = chip_sum(*m0)
        m1 = gated((*h1, *weights), every)
        h2 = residual(2, *a2)
        m1 = chip_sum(*m1)
        m2 = gated((*h2, *weights), every)
        h3 = residual(3, *a2, tokens)
        m2 = chip_sum(*m2)
        r0 = finish(0, (h0[0],), 0, *m0)
        *m3, hidden = gated((*h3, *weights), every[:cut], hidden_out=True)
        m3 = chip_sum(*m3)
        m4 = gated((hidden,), every[cut:])
        r1 = finish(1, (h1[0],), 0, *m1, [put(0, r0)])
        m4 = chip_sum(*m4)
        r2 = finish(2, (h2[0],), 0, *m2, [put(1, r1)])
        r3 = finish(3, (h3[0],), 0, *m3, [put(2, r2)])
        y = run(sums, [put(3, r3)], y, x.shape)[0]
        r4 = finish(3, (h3[0], 0, cut * COLS), cut * COLS, *m4)
        return run(sums, [put(3, r4, cut * COLS)], y, x.shape)[0]

    tokens, whole, columns, rows_of = P("dp", None, None), P(None), P(None, "tp"), P("tp", None)
    return jax.shard_map(
        step,
        mesh=mesh,
        in_specs=(tokens, whole, columns, columns, columns, rows_of, whole, columns, columns, rows_of),
        out_specs=tokens,
        check_vma=False,
    )
```

```python
import functools

import jax
import jax.numpy as jnp
from jax import lax
from jax.experimental import pallas as pl
from jax.experimental.pallas import tpu as pltpu
from jax.sharding import PartitionSpec as P


HEAD = 128
THETA = 10000
LOG2E = 1.4426950408889634
EPS = 1e-6
VMEM = 66_500_000
PANEL = 256
PIECE = 1280
WIDE = 768
COLS = 512

ANY = pl.BlockSpec(memory_space=pl.ANY)


def _call(kernel, token, given, grid, in_specs, out_specs, out_shape, scratch=(), aliases=None, cost=None):
    n, m = len(in_specs), len(out_specs)

    def body(*refs):
        kernel(*refs[: 1 + n], *refs[2 + n : 2 + n + m], *refs[3 + n + m :])

    out = pl.pallas_call(
        body,
        grid_spec=pltpu.PrefetchScalarGridSpec(num_scalar_prefetch=1, grid=grid, in_specs=[*in_specs, ANY], out_specs=[*out_specs, ANY],
                                               scratch_shapes=list(scratch)),
        out_shape=[*out_shape, jax.ShapeDtypeStruct((8, 128), jnp.float32)],
        input_output_aliases=aliases or {},
        compiler_params=pltpu.CompilerParams(dimension_semantics=("arbitrary",) * len(grid), vmem_limit_bytes=VMEM),
        cost_estimate=cost,
    )(*given, token)
    return out[:-1], out[-1]


def _dot(a, b, ca=1, cb=0):
    return lax.dot_general(a, b, (((ca,), (cb,)), ((), ())), preferred_element_type=jnp.float32)


def _once(shape, index_map):
    return pl.BlockSpec(shape, index_map, pipeline_mode=pl.Buffered(1))


def _norm(x_ref, gain_ref, o_ref, rows=64):
    tokens, d = o_ref.shape

    def some(r, _):
        at = pl.ds(pl.multiple_of(r * rows, rows), rows)
        total = jnp.zeros((rows, 128), jnp.float32)
        for c in range(0, d, 128):
            wide = x_ref[at, c : c + 128].astype(jnp.float32)
            total += wide * wide
        scale = lax.rsqrt(jnp.sum(total, -1, keepdims=True) * (1 / d) + EPS)
        for c in range(0, d, 128):
            wide = x_ref[at, c : c + 128].astype(jnp.float32)
            o_ref[at, c : c + 128] = (wide * scale * gain_ref[:, c : c + 128].astype(jnp.float32)).astype(jnp.bfloat16)
        return _

    lax.fori_loop(0, tokens // rows, some, None)


def _rotate(t, cos, sin):
    t = t.astype(jnp.float32)
    return (t * cos + pltpu.roll(t, HEAD // 2, 1) * sin).astype(jnp.bfloat16)


def _scores(q, k):
    half = q.shape[0] // 2
    return [_dot(k[: half * (i + 1)], q[half * i : half * (i + 1)], 1, 1) for i in range(2)]


def _weigh(scores, vt, o_ref, at):
    e = HEAD**-0.5 * LOG2E
    for i, s in enumerate(scores):
        n, half = s.shape
        key = lax.broadcasted_iota(jnp.int32, (half, half), 0)
        query = lax.broadcasted_iota(jnp.int32, (half, half), 1)
        last = jnp.where(query >= key, s[n - half :], -1e30)
        s = jnp.concatenate([s[: n - half], last], 0) if i else last
        top = s.max(axis=0, keepdims=True)
        p = jnp.exp2((s - top) * e).astype(jnp.bfloat16)
        mix = _dot(vt[:, :n], p)
        o = mix[:HEAD] * (1 / mix[HEAD : HEAD + 1])
        o_ref[n - half : n, pl.ds(at, HEAD)] = o.T.astype(jnp.bfloat16)


def _attention_kernel(core_ref, x_hbm, gain_ref, cos_ref, sin_ref, wk_hbm, wv_hbm, wq_hbm, wo_hbm, send_ref, keep_ref,
                      x_s, a_s, q_s, k_s, vt_s, seen_s, wk_s, wv_s, wq_s, wo_s, x_sem, w_sem, *, first, group):
    i = pl.program_id(0)
    tokens, d = a_s.shape
    kvs, nq, no = k_s.shape[0], wq_s.shape[1] // PANEL, wo_s.shape[0]
    per = no // 2

    def fetch(n):
        return pltpu.make_async_copy(x_hbm.at[first + n], x_s, x_sem)

    def copy(n, src, dst):
        return pltpu.make_async_copy(src, dst, w_sem.at[n])

    some = [pl.ds(0, 2 * PANEL), pl.ds(2 * PANEL, (nq - 2) * PANEL)]
    weights = [copy(0, wk_hbm, wk_s), copy(1, wv_hbm, wv_s)] + [copy(2 + n, wq_hbm.at[:, at], wq_s.at[:, at]) for n, at in enumerate(some)]
    for n in range(no):
        half = (1 - core_ref[0]) if n < per else core_ref[0]
        weights.append(copy(4 + n, wo_hbm.at[:, pl.ds(pl.multiple_of((half * per + n % per) * PIECE, PIECE), PIECE)], wo_s.at[n]))

    def ready(n):
        @pl.when(i == 0)
        def _():
            weights[n].wait()

    def begin(these):
        @pl.when(i == 0)
        def _():
            for w in these:
                w.start()

    begin([fetch(0)])
    fetch(i).wait()
    begin(weights[:3])
    _norm(x_s, gain_ref, a_s)
    begin(weights[3:])

    @pl.when(i + 1 < pl.num_programs(0))
    def _():
        fetch(i + 1).start()

    def project(r):
        return _dot(a_s[...], wq_s[:, pl.ds(pl.multiple_of(r * PANEL, PANEL), PANEL)]).astype(jnp.bfloat16)

    def turn(t, r):
        for n in range(2):
            q_s[lax.rem(r, 2), n] = _rotate(t[:, n * HEAD : (n + 1) * HEAD], cos_ref[...], sin_ref[...])

    def attend(r, beside):
        heads = [2 * r + n for n in range(2)]
        kv = [lax.div(head, group) for head in heads]
        scores = [_scores(q_s[lax.rem(r, 2), n], k_s[kv[n]]) for n in range(2)]
        got = beside()
        for n in range(2):
            _weigh(scores[n], vt_s[kv[n]], seen_s, pl.multiple_of(heads[n] * HEAD, HEAD))
        return got

    for n in range(3):
        ready(n)
    t = _dot(a_s[...], wk_s[...]).astype(jnp.bfloat16)
    for n in range(kvs):
        k_s[n] = _rotate(t[:, n * HEAD : (n + 1) * HEAD], cos_ref[...], sin_ref[...])
    t = _dot(a_s[...], wv_s[...])
    for n in range(kvs):
        vt_s[n, :HEAD, :] = t[:, n * HEAD : (n + 1) * HEAD].T.astype(jnp.bfloat16)
        vt_s[n, HEAD:, :] = jnp.ones((16, tokens), jnp.bfloat16)
    turn(project(0), 0)
    ready(3)

    def both(r, _):
        turn(attend(r, lambda: project(r + 1)), r + 1)
        return _

    lax.fori_loop(0, nq - 1, both, None)
    attend(jnp.int32(nq - 1), lambda: None)
    for n in range(no):
        ready(4 + n)
    for n in range(no):
        o_ref = send_ref if n < per else keep_ref
        o_ref[:, n % per * PIECE : (n % per + 1) * PIECE] = _dot(seen_s[...], wo_s[n]).astype(jnp.bfloat16)


def attention_half(token, core, x, gain, cos, sin, wk, wv, wq, wo, first, count):
    _, tokens, d = x.shape
    qd, kvd, half = wq.shape[1], wk.shape[1], d // 2
    no = d // PIECE
    whole = lambda i, core: (0, 0)
    out = jax.ShapeDtypeStruct((count * tokens, half), jnp.bfloat16)
    rows = pl.BlockSpec((tokens, half), lambda i, core: (i, 0))
    return _call(
        functools.partial(_attention_kernel, first=first, group=qd // kvd), token, (core, x, gain, cos, sin, wk, wv, wq, wo), (count,),
        in_specs=[ANY, _once((1, d), whole), _once((tokens, HEAD), whole), _once((tokens, HEAD), whole), ANY, ANY, ANY, ANY],
        out_specs=[rows, rows],
        out_shape=[out, out],
        scratch=[
            pltpu.VMEM((tokens, d), jnp.bfloat16),
            pltpu.VMEM((tokens, d), jnp.bfloat16),
            pltpu.VMEM((2, 2, tokens, HEAD), jnp.bfloat16),
            pltpu.VMEM((kvd // HEAD, tokens, HEAD), jnp.bfloat16),
            pltpu.VMEM((kvd // HEAD, HEAD + 16, tokens), jnp.bfloat16),
            pltpu.VMEM((tokens, qd), jnp.bfloat16),
            pltpu.VMEM((d, kvd), jnp.bfloat16),
            pltpu.VMEM((d, kvd), jnp.bfloat16),
            pltpu.VMEM((d, qd), jnp.bfloat16),
            pltpu.VMEM((no, qd, PIECE), jnp.bfloat16),
            pltpu.SemaphoreType.DMA,
            pltpu.SemaphoreType.DMA((4 + no,)),
        ],
        cost=pl.CostEstimate(
            flops=count * (2 * tokens * d * (2 * qd + 2 * kvd) + 4 * tokens * tokens * qd),
            transcendentals=count * tokens * tokens * qd // HEAD,
            bytes_accessed=2 * (2 * count * tokens * d + d * (2 * qd + 2 * kvd))),
    )


def _mlp_kernel(core_ref, *refs, nf, pieces, count, hidden_in, hidden_out):
    given, refs = (refs[:1], refs[1:]) if hidden_in else (refs[: 2 * count], refs[2 * count :])
    (gain_ref, wg_hbm, wu_hbm), refs = ((None,) * 3, refs) if hidden_in else (refs[:3], refs[3:])
    wd_hbm, refs = refs[0], refs[1:]
    outs, refs = refs[: 2 * count], refs[2 * count :]
    hid_hbm, refs = (refs[0], refs[1:]) if hidden_out else (None, refs)
    w_s, b_s, hid_s, t_s, w_sem, h_sem, t_sem = (refs[0], None, *refs[1:]) if hidden_in else refs
    half = wd_hbm.shape[1] // 2
    per, last = len(pieces), nf + len(pieces)
    seq, j = lax.div(pl.program_id(0), last), lax.rem(pl.program_id(0), last)

    def slot(i, step):
        return 2 * lax.rem(step, 2) + i

    def gate_up(i, step):
        src, at = (wg_hbm, wu_hbm)[i], slot(i, step)
        column = pl.multiple_of(step * WIDE, WIDE)
        return pltpu.make_async_copy(src.at[:, pl.ds(column, WIDE)], w_s.at[at, pl.ds(0, src.shape[0]), :], w_sem.at[at])

    def down(i, step):
        q, at = 2 * (step - nf) + i, slot(i, step)
        core = jnp.where(q < per, 1 - core_ref[0], core_ref[0])
        column = pl.multiple_of(core * half + (lax.rem(q, per) + pieces[0]) * COLS, COLS)
        return pltpu.make_async_copy(wd_hbm.at[:, pl.ds(column, COLS)], w_s.at[at, :, pl.ds(0, COLS)], w_sem.at[at])

    def start(step):
        if nf:
            @pl.when(step < nf)
            def _():
                for i in range(2):
                    gate_up(i, step).start()

        @pl.when((step >= nf) & (step < last))
        def _():
            for i in range(2):
                down(i, step).start()

    def out(q, begin):
        to, at = pl.multiple_of(lax.rem(q, per) * COLS, COLS), lax.rem(q, 4)
        for n, ref in enumerate(outs):
            @pl.when((seq == n // 2) & ((q >= per) if n % 2 else (q < per)))
            def _():
                copy = pltpu.make_async_copy(t_s.at[at], ref.at[:, pl.ds(to, COLS)], t_sem.at[at])
                copy.start() if begin else copy.wait()

    def fetch(n):
        starts = [pl.multiple_of(core * half, 128) for core in (core_ref[0], 1 - core_ref[0])]
        return [pltpu.make_async_copy(ref, b_s.at[:, pl.ds(at, half)], h_sem.at[k])
                for k, (ref, at) in enumerate(zip(given[2 * n : 2 * n + 2], starts))]

    if hidden_in:

        @pl.when(j == 0)
        def _():
            copy = pltpu.make_async_copy(given[0], hid_s, h_sem.at[0])
            copy.start()
            down(0, j).start()
            copy.wait()
            down(1, j).start()
    else:
        for n in range(count):

            @pl.when((seq == n) & (j == 0))
            def _():
                for copy in fetch(n):
                    if n == 0:
                        copy.start()
                for copy in fetch(n):
                    copy.wait()
                if n == 0:
                    start(j)
                _norm(b_s, gain_ref, b_s)

            if n + 1 < count:

                @pl.when((seq == n) & (j == nf))
                def _():
                    for copy in fetch(n + 1):
                        copy.start()

                @pl.when((seq == n) & (j == last - 1))
                def _():
                    start(jnp.int32(0))

    start(j + 1)

    if nf:
        @pl.when(j < nf)
        def _():
            for i in range(2):
                gate_up(i, j).wait()
            d = b_s.shape[1]
            for p in range(WIDE // PANEL):
                at = slice(p * PANEL, (p + 1) * PANEL)
                gate = _dot(b_s[...], w_s[slot(0, j), :d, at])
                up = _dot(b_s[...], w_s[slot(1, j), :d, at])
                to = pl.ds(pl.multiple_of(j * WIDE + p * PANEL, PANEL), PANEL)
                hid_s[:, to] = (gate * jax.nn.sigmoid(gate) * up).astype(jnp.bfloat16)

    if hidden_out:
        put = pltpu.make_async_copy(hid_s, hid_hbm, h_sem.at[0])

        @pl.when(j == nf)
        def _():
            put.start()

    @pl.when(j >= nf)
    def _():
        q = 2 * (j - nf)

        @pl.when(q >= 4)
        def _():
            for i in range(2):
                out(q - 4 + i, False)

        if not hidden_in:
            for i in range(2):
                down(i, j).wait()
        for i in range(2):
            if hidden_in:
                down(i, j).wait()
            t_s[lax.rem(q + i, 4)] = _dot(hid_s[...], w_s[slot(i, j), :, :COLS]).astype(jnp.bfloat16)
        for i in range(2):
            out(q + i, True)

        @pl.when(j == last - 1)
        def _():
            for i in range(-2, 2):
                out(q + i, False)
            if hidden_out:
                put.wait()


def mlp(token, core, given, weights, wd, pieces, hidden_out=False):
    ff, d = wd.shape
    tokens, hidden_in, count = 512, not weights, max(len(given) // 2, 1)
    per = len(pieces)
    nf = 0 if hidden_in else ff // WIDE
    out = jax.ShapeDtypeStruct((tokens, per * COLS), jnp.bfloat16)
    hidden = jax.ShapeDtypeStruct((tokens, ff), jnp.bfloat16)
    flops = count * ((0 if hidden_in else 4 * tokens * d * ff) + 2 * tokens * ff * 2 * per * COLS)
    return _call(
        functools.partial(_mlp_kernel, nf=nf, pieces=pieces, count=count, hidden_in=hidden_in, hidden_out=hidden_out), token,
        (core, *given, *weights, wd), (count * (nf + per),),
        in_specs=[ANY] * len(given) + ([] if hidden_in else [_once((1, d), lambda j, core: (0, 0)), ANY, ANY]) + [ANY],
        out_specs=[ANY] * (2 * count + hidden_out),
        out_shape=[out] * 2 * count + [hidden] * hidden_out,
        scratch=[pltpu.VMEM((4, ff, COLS if hidden_in else WIDE), jnp.bfloat16)]
        + [pltpu.VMEM((tokens, d), jnp.bfloat16)] * (not hidden_in)
        + [
            pltpu.VMEM((tokens, ff), jnp.bfloat16),
            pltpu.VMEM((4, tokens, COLS), jnp.bfloat16),
            pltpu.SemaphoreType.DMA((4,)),
            pltpu.SemaphoreType.DMA((2,)),
            pltpu.SemaphoreType.DMA((4,)),
        ],
        cost=pl.CostEstimate(flops=flops, transcendentals=count * tokens * ff, bytes_accessed=flops // tokens + 4 * count * tokens * d),
    )


def _sums_kernel(core_ref, *refs, jobs, count, fresh, aliased):
    arrays, refs = refs[:count], refs[count:]
    made, refs = refs[: fresh], refs[fresh:]
    y_hbm, refs = (refs[0], refs[1:]) if aliased else (None, refs)
    core = core_ref[0]
    rows = 128
    todo = []
    at_array = at_made = 0
    for seq, terms, keep, to, size, wide in jobs:
        sem, osem, o_s, *t_s = refs[: 3 + len(terms)]
        refs = refs[3 + len(terms) :]
        held = arrays[at_array : at_array + len(terms)]
        at_array += len(terms)
        out = made[at_made] if keep else None
        at_made += bool(keep)
        for r in range(size // rows):
            here = pl.ds(r * rows, rows)
            ins, outs = [], []
            for n, ((row, column), array) in enumerate(zip(terms, held)):
                if len(array.shape) == 3:
                    half = array.shape[2] // 2
                    src = array.at[seq + r * rows // 512, pl.ds(r * rows % 512, rows), pl.ds(pl.multiple_of(core * half, 128), wide)]
                else:
                    src = array.at[pl.ds(row + r * rows, rows), pl.ds(column, wide)]
                ins.append(pltpu.make_async_copy(src, t_s[n].at[here], sem.at[n, r]))
            from_s = o_s if len(terms) > 1 else t_s[0]
            if keep:
                outs.append(pltpu.make_async_copy(from_s.at[here], out.at[here], osem.at[0, r]))
            if to is not None:
                mine, column = to
                half = y_hbm.shape[2] // 2
                start = pl.multiple_of((core if mine else 1 - core) * half + column, 128)
                outs.append(pltpu.make_async_copy(from_s.at[here], y_hbm.at[seq, here, pl.ds(start, wide)], osem.at[1, r]))

            def work(o_s=o_s, t_s=t_s, first=r * rows, rows=rows):
                def some(k, _):
                    at = pl.ds(pl.multiple_of(first + k * 16, 16), 16)
                    total = None
                    for t in t_s[::-1]:
                        t = t[at, :].astype(jnp.float32)
                        total = t if total is None else t + total
                    o_s[at, :] = total.astype(jnp.bfloat16)
                    return _

                if len(t_s) > 1:
                    lax.fori_loop(0, rows // 16, some, None)

            todo.append((ins, outs, work))
    for ins, _, _ in todo:
        for copy in ins:
            copy.start()
    for ins, outs, work in todo:
        for copy in ins:
            copy.wait()
        work()
        for copy in outs:
            copy.start()
    for _, outs, _ in todo:
        for copy in outs:
            copy.wait()


def sums(token, core, jobs, y=None, shape=None):
    given, plain, scratch, out_shape, work = [], [], [], [], 0
    for seq, terms, keep, to in jobs:
        terms = [(t + (0, 0))[:3] for t in terms]
        size, wide = terms[-1][0].shape
        size = min(size, 512)
        given += [t[0] for t in terms]
        plain.append((seq, [t[1:] for t in terms], keep, to, size, wide))
        buffer = pltpu.VMEM((size, wide), jnp.bfloat16)
        scratch += [pltpu.SemaphoreType.DMA((len(terms), size // 128)), pltpu.SemaphoreType.DMA((2, size // 128))]
        scratch += [buffer if len(terms) > 1 else pltpu.VMEM((16, 128), jnp.bfloat16)] + [buffer] * len(terms)
        out_shape += [jax.ShapeDtypeStruct((size, wide), jnp.bfloat16)] * bool(keep)
        work += (len(terms) + 1) * size * wide
    count, fresh = len(given), len(out_shape)
    aliased = any(to is not None for *_, to in jobs)
    if aliased:
        out_shape.append(jax.ShapeDtypeStruct(shape, jnp.bfloat16))
    had = aliased and y is not None

    def kernel(core_ref, *refs):
        _sums_kernel(core_ref, *refs[:count], *refs[count + had :], jobs=plain, count=count, fresh=fresh, aliased=aliased)

    out, token = _call(
        kernel, token, (core, *given, *([y] if had else [])), (1,),
        in_specs=[ANY] * (count + had),
        out_specs=[ANY] * len(out_shape),
        out_shape=out_shape,
        scratch=scratch,
        aliases={1 + count: fresh} if had else None,
        cost=pl.CostEstimate(flops=work, transcendentals=0, bytes_accessed=2 * work),
    )
    return tuple(out), token


def solution(mesh):
    n = mesh.shape["tp"]
    core_pairs = [(i, i ^ 1) for i in range(n)]
    chip_pairs = [(i, i ^ 2) for i in range(n)]

    def step(x, gain_a, wq, wk, wv, wo, gain_m, w_gate, w_up, w_down):
        tokens, d = x.shape[1:]
        core = lax.rem(lax.axis_index("tp"), 2).reshape(1)
        angle = jnp.arange(tokens, dtype=jnp.float32)[:, None] * THETA ** (-(jnp.arange(HEAD) % (HEAD // 2)).astype(jnp.float32) / (HEAD // 2))
        cos, sin = jnp.cos(angle), jnp.sin(angle) * jnp.where(jnp.arange(HEAD) < HEAD // 2, -1.0, 1.0)
        gain_a, gain_m = gain_a.reshape(1, d), gain_m.reshape(1, d)
        token, y = cos, None

        def run(f, *args, **more):
            nonlocal token
            out, token = f(token, core, *args, **more)
            return out

        def send(pairs, array):
            return lax.ppermute(array, "tp", pairs)

        def attention(s, count=1):
            out, keep = run(attention_half, x, gain_a, cos, sin, wk, wv, wq, wo, s, count)
            return send(core_pairs, out), keep

        def gated(given, pieces, **more):
            out = run(mlp, given, weights, w_down, pieces, **more)
            return (send(core_pairs, out[0]), *out[1:])

        def chip_sum(came, keep):
            (term,) = run(sums, [(0, [(keep,), (came,)], True, None)])
            return term, send(chip_pairs, term)

        def residual(s, term, came):
            (own,) = run(sums, [(s, [(x,), (term,), (came,)], True, None)])
            return own, send(core_pairs, own)

        def finish(s, base, column, term, came, others=()):
            nonlocal y
            mine = (s, [base, (term,), (came,)], True, (True, column))
            own, y = run(sums, [mine, *others], y, x.shape)
            return send(core_pairs, own)

        def put(s, came, column=0):
            return s, [(came,)], False, (False, column)

        weights = gain_m, w_gate, w_up
        every = tuple(range(d // 2 // COLS))
        cut = 3
        a0 = attention(0)
        a1 = attention(1)
        a0 = chip_sum(*a0)
        came, keep = attention(2, 2)
        a1 = chip_sum(*a1)
        h0 = residual(0, *a0)
        a2, a3 = run(sums, [(0, [(keep, n * tokens), (came, n * tokens)], True, None) for n in range(2)])
        a2, a3 = (a2, send(chip_pairs, a2)), (a3, send(chip_pairs, a3))
        m0 = gated(h0, every)
        h1 = residual(1, *a1)
        h2 = residual(2, *a2)
        m0 = chip_sum(*m0)
        out = run(mlp, (*h1, *h2), weights, w_down, every)
        m1, m2 = (send(core_pairs, out[0]), out[1]), (send(core_pairs, out[2]), out[3])
        h3 = residual(3, *a3)
        m1 = chip_sum(*m1)
        m2 = chip_sum(*m2)
        *m3, hidden = gated(h3, every[:cut], hidden_out=True)
        m3 = chip_sum(*m3)
        came = run(mlp, (hidden,), (), w_down, every[cut:])
        m4 = send(core_pairs, came[0]), came[1]
        r0 = finish(0, (h0[0],), 0, *m0)
        m4 = chip_sum(*m4)
        r1 = finish(1, (h1[0],), 0, *m1, [put(0, r0)])
        r2 = finish(2, (h2[0],), 0, *m2, [put(1, r1)])
        r3 = finish(3, (h3[0],), 0, *m3, [put(2, r2)])
        y = run(sums, [put(3, r3)], y, x.shape)[0]
        r4 = finish(3, (h3[0], 0, cut * COLS), cut * COLS, *m4)
        return run(sums, [put(3, r4, cut * COLS)], y, x.shape)[0]

    tokens, whole, columns, rows_of = P("dp", None, None), P(None), P(None, "tp"), P("tp", None)
    return jax.shard_map(
        step,
        mesh=mesh,
        in_specs=(tokens, whole, columns, columns, columns, rows_of, whole, columns, columns, rows_of),
        out_specs=tokens,
        check_vma=False,
    )
```

```python
import functools

import jax
import jax.numpy as jnp
from jax import lax
from jax.experimental import pallas as pl
from jax.experimental.pallas import tpu as pltpu
from jax.sharding import PartitionSpec as P


HEAD = 128
THETA = 10000
LOG2E = 1.4426950408889634
EPS = 1e-6
VMEM = 66_500_000
PANEL = 256
PIECE = 1280
WIDE = 768
COLS = 512

ANY = pl.BlockSpec(memory_space=pl.ANY)


def _call(kernel, token, given, grid, in_specs, out_specs, out_shape, scratch=(), aliases=None, cost=None):
    n, m = len(in_specs), len(out_specs)

    def body(*refs):
        kernel(*refs[: 1 + n], *refs[2 + n : 2 + n + m], *refs[3 + n + m :])

    out = pl.pallas_call(
        body,
        grid_spec=pltpu.PrefetchScalarGridSpec(num_scalar_prefetch=1, grid=grid, in_specs=[*in_specs, ANY], out_specs=[*out_specs, ANY],
                                               scratch_shapes=list(scratch)),
        out_shape=[*out_shape, jax.ShapeDtypeStruct((8, 128), jnp.float32)],
        input_output_aliases=aliases or {},
        compiler_params=pltpu.CompilerParams(dimension_semantics=("arbitrary",) * len(grid), vmem_limit_bytes=VMEM),
        cost_estimate=cost,
    )(*given, token)
    return out[:-1], out[-1]


def _dot(a, b, ca=1, cb=0):
    return lax.dot_general(a, b, (((ca,), (cb,)), ((), ())), preferred_element_type=jnp.float32)


def _once(shape, index_map):
    return pl.BlockSpec(shape, index_map, pipeline_mode=pl.Buffered(1))


def _norm(x_ref, gain_ref, o_ref, rows=64):
    tokens, d = o_ref.shape

    def some(r, _):
        at = pl.ds(pl.multiple_of(r * rows, rows), rows)
        total = jnp.zeros((rows, 128), jnp.float32)
        for c in range(0, d, 128):
            wide = x_ref[at, c : c + 128].astype(jnp.float32)
            total += wide * wide
        scale = lax.rsqrt(jnp.sum(total, -1, keepdims=True) * (1 / d) + EPS)
        for c in range(0, d, 128):
            wide = x_ref[at, c : c + 128].astype(jnp.float32)
            o_ref[at, c : c + 128] = (wide * scale * gain_ref[:, c : c + 128].astype(jnp.float32)).astype(jnp.bfloat16)
        return _

    lax.fori_loop(0, tokens // rows, some, None)


def _rotate(t, cos, sin):
    t = t.astype(jnp.float32)
    return (t * cos + pltpu.roll(t, HEAD // 2, 1) * sin).astype(jnp.bfloat16)


def _scores(q, k):
    half = q.shape[0] // 2
    return [_dot(k[: half * (i + 1)], q[half * i : half * (i + 1)], 1, 1) for i in range(2)]


def _weigh(scores, p_ref):
    e = HEAD**-0.5 * LOG2E
    at = 0
    for i, s in enumerate(scores):
        n, half = s.shape
        key = lax.broadcasted_iota(jnp.int32, (half, half), 0)
        query = lax.broadcasted_iota(jnp.int32, (half, half), 1)
        last = jnp.where(query >= key, s[n - half :], -1e30)
        s = jnp.concatenate([s[: n - half], last], 0) if i else last
        top = s.max(axis=0, keepdims=True)
        p_ref[at : at + n, :] = jnp.exp2((s - top) * e).astype(jnp.bfloat16)
        at += n


def _mix(p_ref, vt, o_ref, column):
    half = p_ref.shape[1]
    at = 0
    for i in range(2):
        n = half * (i + 1)
        mix = _dot(vt[:, :n], p_ref[at : at + n, :])
        o = mix[:HEAD] * (1 / mix[HEAD : HEAD + 1])
        o_ref[half * i : n, pl.ds(column, HEAD)] = o.T.astype(jnp.bfloat16)
        at += n


def _attention_kernel(core_ref, x_hbm, gain_ref, cos_ref, sin_ref, wk_hbm, wv_hbm, wq_hbm, wo_hbm, send_ref, keep_ref,
                      x_s, a_s, q_s, k_s, vt_s, p_s, seen_s, wk_s, wv_s, wq_s, wo_s, x_sem, w_sem, *, first, group):
    i = pl.program_id(0)
    tokens, d = a_s.shape
    kvs, nq, no = k_s.shape[0], wq_s.shape[1] // PANEL, wo_s.shape[0]
    per = no // 2

    def fetch(n):
        return pltpu.make_async_copy(x_hbm.at[first + n], x_s, x_sem)

    def copy(n, src, dst):
        return pltpu.make_async_copy(src, dst, w_sem.at[n])

    some = [pl.ds(0, 2 * PANEL), pl.ds(2 * PANEL, (nq - 2) * PANEL)]
    weights = [copy(0, wk_hbm, wk_s), copy(1, wv_hbm, wv_s)] + [copy(2 + n, wq_hbm.at[:, at], wq_s.at[:, at]) for n, at in enumerate(some)]
    for n in range(no):
        half = (1 - core_ref[0]) if n < per else core_ref[0]
        weights.append(copy(4 + n, wo_hbm.at[:, pl.ds(pl.multiple_of((half * per + n % per) * PIECE, PIECE), PIECE)], wo_s.at[n]))

    def ready(n):
        @pl.when(i == 0)
        def _():
            weights[n].wait()

    def begin(these):
        @pl.when(i == 0)
        def _():
            for w in these:
                w.start()

    begin([fetch(0)])
    fetch(i).wait()
    begin(weights[:3])
    _norm(x_s, gain_ref, a_s)
    begin(weights[3:])

    @pl.when(i + 1 < pl.num_programs(0))
    def _():
        fetch(i + 1).start()

    def project(r):
        return _dot(a_s[...], wq_s[:, pl.ds(pl.multiple_of(r * PANEL, PANEL), PANEL)]).astype(jnp.bfloat16)

    def turn(t, r):
        for n in range(2):
            q_s[lax.rem(r, 2), n] = _rotate(t[:, n * HEAD : (n + 1) * HEAD], cos_ref[...], sin_ref[...])

    def kv(r, n):
        return lax.div(2 * r + n, group)

    def score(r):
        return [_scores(q_s[lax.rem(r, 2), n], k_s[kv(r, n)]) for n in range(2)]

    def weigh(scores):
        for n in range(2):
            _weigh(scores[n], p_s.at[n])

    def mix(r):
        for n in range(2):
            _mix(p_s.at[n], vt_s[kv(r, n)], seen_s, pl.multiple_of((2 * r + n) * HEAD, HEAD))

    for n in range(3):
        ready(n)
    t = _dot(a_s[...], wk_s[...]).astype(jnp.bfloat16)
    for n in range(kvs):
        k_s[n] = _rotate(t[:, n * HEAD : (n + 1) * HEAD], cos_ref[...], sin_ref[...])
    t = _dot(a_s[...], wv_s[...])
    for n in range(kvs):
        vt_s[n, :HEAD, :] = t[:, n * HEAD : (n + 1) * HEAD].T.astype(jnp.bfloat16)
        vt_s[n, HEAD:, :] = jnp.ones((16, tokens), jnp.bfloat16)
    turn(project(0), 0)
    ready(3)

    def stage(r, before=True):
        if before:
            mix(r - 1)
        scores = score(r)
        t = project(r + 1)
        weigh(scores)
        turn(t, r + 1)

    stage(jnp.int32(0), False)
    lax.fori_loop(1, nq - 1, lambda r, _: stage(r), None)
    mix(jnp.int32(nq - 2))
    weigh(score(jnp.int32(nq - 1)))
    mix(jnp.int32(nq - 1))
    for n in range(no):
        ready(4 + n)
    for n in range(no):
        o_ref = send_ref if n < per else keep_ref
        o_ref[:, n % per * PIECE : (n % per + 1) * PIECE] = _dot(seen_s[...], wo_s[n]).astype(jnp.bfloat16)


def attention_half(token, core, x, gain, cos, sin, wk, wv, wq, wo, first, count):
    _, tokens, d = x.shape
    qd, kvd, half = wq.shape[1], wk.shape[1], d // 2
    no = d // PIECE
    whole = lambda i, core: (0, 0)
    out = jax.ShapeDtypeStruct((count * tokens, half), jnp.bfloat16)
    rows = pl.BlockSpec((tokens, half), lambda i, core: (i, 0))
    return _call(
        functools.partial(_attention_kernel, first=first, group=qd // kvd), token, (core, x, gain, cos, sin, wk, wv, wq, wo), (count,),
        in_specs=[ANY, _once((1, d), whole), _once((tokens, HEAD), whole), _once((tokens, HEAD), whole), ANY, ANY, ANY, ANY],
        out_specs=[rows, rows],
        out_shape=[out, out],
        scratch=[
            pltpu.VMEM((tokens, d), jnp.bfloat16),
            pltpu.VMEM((tokens, d), jnp.bfloat16),
            pltpu.VMEM((2, 2, tokens, HEAD), jnp.bfloat16),
            pltpu.VMEM((kvd // HEAD, tokens, HEAD), jnp.bfloat16),
            pltpu.VMEM((kvd // HEAD, HEAD + 16, tokens), jnp.bfloat16),
            pltpu.VMEM((2, tokens * 3 // 2, tokens // 2), jnp.bfloat16),
            pltpu.VMEM((tokens, qd), jnp.bfloat16),
            pltpu.VMEM((d, kvd), jnp.bfloat16),
            pltpu.VMEM((d, kvd), jnp.bfloat16),
            pltpu.VMEM((d, qd), jnp.bfloat16),
            pltpu.VMEM((no, qd, PIECE), jnp.bfloat16),
            pltpu.SemaphoreType.DMA,
            pltpu.SemaphoreType.DMA((4 + no,)),
        ],
        cost=pl.CostEstimate(
            flops=count * (2 * tokens * d * (2 * qd + 2 * kvd) + 4 * tokens * tokens * qd),
            transcendentals=count * tokens * tokens * qd // HEAD,
            bytes_accessed=2 * (2 * count * tokens * d + d * (2 * qd + 2 * kvd))),
    )


def _mlp_kernel(core_ref, *refs, nf, pieces, count, hidden_in, hidden_out):
    given, refs = (refs[:1], refs[1:]) if hidden_in else (refs[: 2 * count], refs[2 * count :])
    (gain_ref, wg_hbm, wu_hbm), refs = ((None,) * 3, refs) if hidden_in else (refs[:3], refs[3:])
    wd_hbm, refs = refs[0], refs[1:]
    outs, refs = refs[: 2 * count], refs[2 * count :]
    hid_hbm, refs = (refs[0], refs[1:]) if hidden_out else (None, refs)
    w_s, b_s, hid_s, t_s, w_sem, h_sem, t_sem = (refs[0], None, *refs[1:]) if hidden_in else refs
    half = wd_hbm.shape[1] // 2
    per, last = len(pieces), nf + len(pieces)
    seq, j = lax.div(pl.program_id(0), last), lax.rem(pl.program_id(0), last)

    def slot(i, step):
        return 2 * lax.rem(step, 2) + i

    def gate_up(i, step):
        src, at = (wg_hbm, wu_hbm)[i], slot(i, step)
        column = pl.multiple_of(step * WIDE, WIDE)
        return pltpu.make_async_copy(src.at[:, pl.ds(column, WIDE)], w_s.at[at, pl.ds(0, src.shape[0]), :], w_sem.at[at])

    def down(i, step):
        q, at = 2 * (step - nf) + i, slot(i, step)
        core = jnp.where(q < per, 1 - core_ref[0], core_ref[0])
        column = pl.multiple_of(core * half + (lax.rem(q, per) + pieces[0]) * COLS, COLS)
        return pltpu.make_async_copy(wd_hbm.at[:, pl.ds(column, COLS)], w_s.at[at, :, pl.ds(0, COLS)], w_sem.at[at])

    def start(step):
        if nf:
            @pl.when(step < nf)
            def _():
                for i in range(2):
                    gate_up(i, step).start()

        @pl.when((step >= nf) & (step < last))
        def _():
            for i in range(2):
                down(i, step).start()

    def out(q, begin):
        to, at = pl.multiple_of(lax.rem(q, per) * COLS, COLS), lax.rem(q, 4)
        for n, ref in enumerate(outs):
            @pl.when((seq == n // 2) & ((q >= per) if n % 2 else (q < per)))
            def _():
                copy = pltpu.make_async_copy(t_s.at[at], ref.at[:, pl.ds(to, COLS)], t_sem.at[at])
                copy.start() if begin else copy.wait()

    def fetch(n):
        starts = [pl.multiple_of(core * half, 128) for core in (core_ref[0], 1 - core_ref[0])]
        return [pltpu.make_async_copy(ref, b_s.at[:, pl.ds(at, half)], h_sem.at[k])
                for k, (ref, at) in enumerate(zip(given[2 * n : 2 * n + 2], starts))]

    if hidden_in:

        @pl.when(j == 0)
        def _():
            copy = pltpu.make_async_copy(given[0], hid_s, h_sem.at[0])
            copy.start()
            down(0, j).start()
            copy.wait()
            down(1, j).start()
    else:
        for n in range(count):

            @pl.when((seq == n) & (j == 0))
            def _():
                for copy in fetch(n):
                    if n == 0:
                        copy.start()
                for copy in fetch(n):
                    copy.wait()
                if n == 0:
                    start(j)
                _norm(b_s, gain_ref, b_s)

            if n + 1 < count:

                @pl.when((seq == n) & (j == nf))
                def _():
                    for copy in fetch(n + 1):
                        copy.start()

                @pl.when((seq == n) & (j == last - 1))
                def _():
                    start(jnp.int32(0))

    start(j + 1)

    if nf:
        @pl.when(j < nf)
        def _():
            for i in range(2):
                gate_up(i, j).wait()
            d = b_s.shape[1]
            for p in range(WIDE // PANEL):
                at = slice(p * PANEL, (p + 1) * PANEL)
                gate = _dot(b_s[...], w_s[slot(0, j), :d, at])
                up = _dot(b_s[...], w_s[slot(1, j), :d, at])
                to = pl.ds(pl.multiple_of(j * WIDE + p * PANEL, PANEL), PANEL)
                hid_s[:, to] = (gate * jax.nn.sigmoid(gate) * up).astype(jnp.bfloat16)

    if hidden_out:
        put = pltpu.make_async_copy(hid_s, hid_hbm, h_sem.at[0])

        @pl.when(j == nf)
        def _():
            put.start()

    @pl.when(j >= nf)
    def _():
        q = 2 * (j - nf)

        @pl.when(q >= 4)
        def _():
            for i in range(2):
                out(q - 4 + i, False)

        if not hidden_in:
            for i in range(2):
                down(i, j).wait()
        for i in range(2):
            if hidden_in:
                down(i, j).wait()
            t_s[lax.rem(q + i, 4)] = _dot(hid_s[...], w_s[slot(i, j), :, :COLS]).astype(jnp.bfloat16)
        for i in range(2):
            out(q + i, True)

        @pl.when(j == last - 1)
        def _():
            for i in range(-2, 2):
                out(q + i, False)
            if hidden_out:
                put.wait()


def mlp(token, core, given, weights, wd, pieces, hidden_out=False):
    ff, d = wd.shape
    tokens, hidden_in, count = 512, not weights, max(len(given) // 2, 1)
    per = len(pieces)
    nf = 0 if hidden_in else ff // WIDE
    out = jax.ShapeDtypeStruct((tokens, per * COLS), jnp.bfloat16)
    hidden = jax.ShapeDtypeStruct((tokens, ff), jnp.bfloat16)
    flops = count * ((0 if hidden_in else 4 * tokens * d * ff) + 2 * tokens * ff * 2 * per * COLS)
    return _call(
        functools.partial(_mlp_kernel, nf=nf, pieces=pieces, count=count, hidden_in=hidden_in, hidden_out=hidden_out), token,
        (core, *given, *weights, wd), (count * (nf + per),),
        in_specs=[ANY] * len(given) + ([] if hidden_in else [_once((1, d), lambda j, core: (0, 0)), ANY, ANY]) + [ANY],
        out_specs=[ANY] * (2 * count + hidden_out),
        out_shape=[out] * 2 * count + [hidden] * hidden_out,
        scratch=[pltpu.VMEM((4, ff, COLS if hidden_in else WIDE), jnp.bfloat16)]
        + [pltpu.VMEM((tokens, d), jnp.bfloat16)] * (not hidden_in)
        + [
            pltpu.VMEM((tokens, ff), jnp.bfloat16),
            pltpu.VMEM((4, tokens, COLS), jnp.bfloat16),
            pltpu.SemaphoreType.DMA((4,)),
            pltpu.SemaphoreType.DMA((2,)),
            pltpu.SemaphoreType.DMA((4,)),
        ],
        cost=pl.CostEstimate(flops=flops, transcendentals=count * tokens * ff, bytes_accessed=flops // tokens + 4 * count * tokens * d),
    )


def _sums_kernel(core_ref, *refs, jobs, count, fresh, aliased):
    arrays, refs = refs[:count], refs[count:]
    made, refs = refs[: fresh], refs[fresh:]
    y_hbm, refs = (refs[0], refs[1:]) if aliased else (None, refs)
    core = core_ref[0]
    rows = 128
    todo = []
    at_array = at_made = 0
    for seq, terms, keep, to, size, wide in jobs:
        sem, osem, o_s, *t_s = refs[: 3 + len(terms)]
        refs = refs[3 + len(terms) :]
        held = arrays[at_array : at_array + len(terms)]
        at_array += len(terms)
        out = made[at_made] if keep else None
        at_made += bool(keep)
        for r in range(size // rows):
            here = pl.ds(r * rows, rows)
            ins, outs = [], []
            for n, ((row, column), array) in enumerate(zip(terms, held)):
                if len(array.shape) == 3:
                    half = array.shape[2] // 2
                    src = array.at[seq + r * rows // 512, pl.ds(r * rows % 512, rows), pl.ds(pl.multiple_of(core * half, 128), wide)]
                else:
                    src = array.at[pl.ds(row + r * rows, rows), pl.ds(column, wide)]
                ins.append(pltpu.make_async_copy(src, t_s[n].at[here], sem.at[n, r]))
            from_s = o_s if len(terms) > 1 else t_s[0]
            if keep:
                outs.append(pltpu.make_async_copy(from_s.at[here], out.at[here], osem.at[0, r]))
            if to is not None:
                mine, column = to
                half = y_hbm.shape[2] // 2
                start = pl.multiple_of((core if mine else 1 - core) * half + column, 128)
                outs.append(pltpu.make_async_copy(from_s.at[here], y_hbm.at[seq, here, pl.ds(start, wide)], osem.at[1, r]))

            def work(o_s=o_s, t_s=t_s, first=r * rows, rows=rows):
                def some(k, _):
                    at = pl.ds(pl.multiple_of(first + k * 16, 16), 16)
                    total = None
                    for t in t_s[::-1]:
                        t = t[at, :].astype(jnp.float32)
                        total = t if total is None else t + total
                    o_s[at, :] = total.astype(jnp.bfloat16)
                    return _

                if len(t_s) > 1:
                    lax.fori_loop(0, rows // 16, some, None)

            todo.append((ins, outs, work))
    for ins, _, _ in todo:
        for copy in ins:
            copy.start()
    for ins, outs, work in todo:
        for copy in ins:
            copy.wait()
        work()
        for copy in outs:
            copy.start()
    for _, outs, _ in todo:
        for copy in outs:
            copy.wait()


def sums(token, core, jobs, y=None, shape=None):
    given, plain, scratch, out_shape, work = [], [], [], [], 0
    for seq, terms, keep, to in jobs:
        terms = [(t + (0, 0))[:3] for t in terms]
        size, wide = terms[-1][0].shape
        size = min(size, 512)
        given += [t[0] for t in terms]
        plain.append((seq, [t[1:] for t in terms], keep, to, size, wide))
        buffer = pltpu.VMEM((size, wide), jnp.bfloat16)
        scratch += [pltpu.SemaphoreType.DMA((len(terms), size // 128)), pltpu.SemaphoreType.DMA((2, size // 128))]
        scratch += [buffer if len(terms) > 1 else pltpu.VMEM((16, 128), jnp.bfloat16)] + [buffer] * len(terms)
        out_shape += [jax.ShapeDtypeStruct((size, wide), jnp.bfloat16)] * bool(keep)
        work += (len(terms) + 1) * size * wide
    count, fresh = len(given), len(out_shape)
    aliased = any(to is not None for *_, to in jobs)
    if aliased:
        out_shape.append(jax.ShapeDtypeStruct(shape, jnp.bfloat16))
    had = aliased and y is not None

    def kernel(core_ref, *refs):
        _sums_kernel(core_ref, *refs[:count], *refs[count + had :], jobs=plain, count=count, fresh=fresh, aliased=aliased)

    out, token = _call(
        kernel, token, (core, *given, *([y] if had else [])), (1,),
        in_specs=[ANY] * (count + had),
        out_specs=[ANY] * len(out_shape),
        out_shape=out_shape,
        scratch=scratch,
        aliases={1 + count: fresh} if had else None,
        cost=pl.CostEstimate(flops=work, transcendentals=0, bytes_accessed=2 * work),
    )
    return tuple(out), token


def solution(mesh):
    n = mesh.shape["tp"]
    core_pairs = [(i, i ^ 1) for i in range(n)]
    chip_pairs = [(i, i ^ 2) for i in range(n)]

    def step(x, gain_a, wq, wk, wv, wo, gain_m, w_gate, w_up, w_down):
        tokens, d = x.shape[1:]
        core = lax.rem(lax.axis_index("tp"), 2).reshape(1)
        angle = jnp.arange(tokens, dtype=jnp.float32)[:, None] * THETA ** (-(jnp.arange(HEAD) % (HEAD // 2)).astype(jnp.float32) / (HEAD // 2))
        cos, sin = jnp.cos(angle), jnp.sin(angle) * jnp.where(jnp.arange(HEAD) < HEAD // 2, -1.0, 1.0)
        gain_a, gain_m = gain_a.reshape(1, d), gain_m.reshape(1, d)
        token, y = cos, None

        def run(f, *args, **more):
            nonlocal token
            out, token = f(token, core, *args, **more)
            return out

        def send(pairs, array):
            return lax.ppermute(array, "tp", pairs)

        def attention(s, count=1):
            out, keep = run(attention_half, x, gain_a, cos, sin, wk, wv, wq, wo, s, count)
            return send(core_pairs, out), keep

        def gated(given, pieces, **more):
            out = run(mlp, given, weights, w_down, pieces, **more)
            return (send(core_pairs, out[0]), *out[1:])

        def chip_sum(came, keep):
            (term,) = run(sums, [(0, [(keep,), (came,)], True, None)])
            return term, send(chip_pairs, term)

        def residual(s, term, came):
            (own,) = run(sums, [(s, [(x,), (term,), (came,)], True, None)])
            return own, send(core_pairs, own)

        def finish(s, base, column, term, came, others=()):
            nonlocal y
            mine = (s, [base, (term,), (came,)], True, (True, column))
            own, y = run(sums, [mine, *others], y, x.shape)
            return send(core_pairs, own)

        def put(s, came, column=0):
            return s, [(came,)], False, (False, column)

        weights = gain_m, w_gate, w_up
        every = tuple(range(d // 2 // COLS))
        cut = 3
        a0 = attention(0)
        a1 = attention(1)
        a0 = chip_sum(*a0)
        came, keep = attention(2, 2)
        a1 = chip_sum(*a1)
        h0 = residual(0, *a0)
        a2, a3 = run(sums, [(0, [(keep, n * tokens), (came, n * tokens)], True, None) for n in range(2)])
        a2, a3 = (a2, send(chip_pairs, a2)), (a3, send(chip_pairs, a3))
        m0 = gated(h0, every)
        h1 = residual(1, *a1)
        h2 = residual(2, *a2)
        m0 = chip_sum(*m0)
        out = run(mlp, (*h1, *h2), weights, w_down, every)
        m1, m2 = (send(core_pairs, out[0]), out[1]), (send(core_pairs, out[2]), out[3])
        h3 = residual(3, *a3)
        m1 = chip_sum(*m1)
        m2 = chip_sum(*m2)
        *m3, hidden = gated(h3, every[:cut], hidden_out=True)
        m3 = chip_sum(*m3)
        came = run(mlp, (hidden,), (), w_down, every[cut:])
        m4 = send(core_pairs, came[0]), came[1]
        r0 = finish(0, (h0[0],), 0, *m0)
        m4 = chip_sum(*m4)
        r1 = finish(1, (h1[0],), 0, *m1)
        r2 = finish(2, (h2[0],), 0, *m2)
        y = run(sums, [put(0, r0), put(1, r1)], y, x.shape)[0]
        r3 = finish(3, (h3[0],), 0, *m3, [put(2, r2)])
        r4 = finish(3, (h3[0], 0, cut * COLS), cut * COLS, *m4)
        return run(sums, [put(3, r3), put(3, r4, cut * COLS)], y, x.shape)[0]

    tokens, whole, columns, rows_of = P("dp", None, None), P(None), P(None, "tp"), P("tp", None)
    return jax.shard_map(
        step,
        mesh=mesh,
        in_specs=(tokens, whole, columns, columns, columns, rows_of, whole, columns, columns, rows_of),
        out_specs=tokens,
        check_vma=False,
    )
```

```python
import functools

import jax
import jax.numpy as jnp
from jax import lax
from jax.experimental import pallas as pl
from jax.experimental.pallas import tpu as pltpu
from jax.sharding import PartitionSpec as P


HEAD = 128
THETA = 10000
LOG2E = 1.4426950408889634
EPS = 1e-6
VMEM = 66_500_000
PANEL = 256
PIECE = 1280
WIDE = 768
COLS = 512

ANY = pl.BlockSpec(memory_space=pl.ANY)


def _call(kernel, token, given, grid, in_specs, out_specs, out_shape, scratch=(), aliases=None, cost=None):
    n, m = len(in_specs), len(out_specs)

    def body(*refs):
        kernel(*refs[: 1 + n], *refs[2 + n : 2 + n + m], *refs[3 + n + m :])

    out = pl.pallas_call(
        body,
        grid_spec=pltpu.PrefetchScalarGridSpec(num_scalar_prefetch=1, grid=grid, in_specs=[*in_specs, ANY], out_specs=[*out_specs, ANY],
                                               scratch_shapes=list(scratch)),
        out_shape=[*out_shape, jax.ShapeDtypeStruct((8, 128), jnp.float32)],
        input_output_aliases=aliases or {},
        compiler_params=pltpu.CompilerParams(dimension_semantics=("arbitrary",) * len(grid), vmem_limit_bytes=VMEM),
        cost_estimate=cost,
    )(*given, token)
    return out[:-1], out[-1]


def _dot(a, b, ca=1, cb=0):
    return lax.dot_general(a, b, (((ca,), (cb,)), ((), ())), preferred_element_type=jnp.float32)


def _once(shape, index_map):
    return pl.BlockSpec(shape, index_map, pipeline_mode=pl.Buffered(1))


def _norm(x_ref, gain_ref, o_ref, rows=64):
    tokens, d = o_ref.shape

    def some(r, _):
        at = pl.ds(pl.multiple_of(r * rows, rows), rows)
        total = jnp.zeros((rows, 128), jnp.float32)
        for c in range(0, d, 128):
            wide = x_ref[at, c : c + 128].astype(jnp.float32)
            total += wide * wide
        scale = lax.rsqrt(jnp.sum(total, -1, keepdims=True) * (1 / d) + EPS)
        for c in range(0, d, 128):
            wide = x_ref[at, c : c + 128].astype(jnp.float32)
            o_ref[at, c : c + 128] = (wide * scale * gain_ref[:, c : c + 128].astype(jnp.float32)).astype(jnp.bfloat16)
        return _

    lax.fori_loop(0, tokens // rows, some, None)


def _rotate(t, cos, sin):
    t = t.astype(jnp.float32)
    return (t * cos + pltpu.roll(t, HEAD // 2, 1) * sin).astype(jnp.bfloat16)


def _scores(q, k):
    half = q.shape[0] // 2
    return [_dot(k[: half * (i + 1)], q[half * i : half * (i + 1)], 1, 1) for i in range(2)]


def _weigh(scores, vt, o_ref, at):
    e = HEAD**-0.5 * LOG2E
    for i, s in enumerate(scores):
        n, half = s.shape
        key = lax.broadcasted_iota(jnp.int32, (half, half), 0)
        query = lax.broadcasted_iota(jnp.int32, (half, half), 1)
        last = jnp.where(query >= key, s[n - half :], -1e30)
        s = jnp.concatenate([s[: n - half], last], 0) if i else last
        top = s.max(axis=0, keepdims=True)
        p = jnp.exp2((s - top) * e).astype(jnp.bfloat16)
        mix = _dot(vt[:, :n], p)
        o = mix[:HEAD] * (1 / mix[HEAD : HEAD + 1])
        o_ref[n - half : n, pl.ds(at, HEAD)] = o.T.astype(jnp.bfloat16)


def _attention_kernel(core_ref, x_hbm, gain_ref, cos_ref, sin_ref, wk_hbm, wv_hbm, wq_hbm, wo_hbm, send_ref, keep_ref,
                      x_s, a_s, q_s, k_s, vt_s, seen_s, wk_s, wv_s, wq_s, wo_s, x_sem, w_sem, *, first, group):
    i = pl.program_id(0)
    tokens, d = a_s.shape
    kvs, nq, no = k_s.shape[0], wq_s.shape[1] // PANEL, wo_s.shape[0]
    per = no // 2

    def fetch(n):
        return pltpu.make_async_copy(x_hbm.at[first + n], x_s, x_sem)

    def copy(n, src, dst):
        return pltpu.make_async_copy(src, dst, w_sem.at[n])

    some = [pl.ds(0, 2 * PANEL), pl.ds(2 * PANEL, (nq - 2) * PANEL)]
    weights = [copy(0, wk_hbm, wk_s), copy(1, wv_hbm, wv_s)] + [copy(2 + n, wq_hbm.at[:, at], wq_s.at[:, at]) for n, at in enumerate(some)]
    for n in range(no):
        half = (1 - core_ref[0]) if n < per else core_ref[0]
        weights.append(copy(4 + n, wo_hbm.at[:, pl.ds(pl.multiple_of((half * per + n % per) * PIECE, PIECE), PIECE)], wo_s.at[n]))

    def ready(n):
        @pl.when(i == 0)
        def _():
            weights[n].wait()

    def begin(these):
        @pl.when(i == 0)
        def _():
            for w in these:
                w.start()

    begin([fetch(0)])
    fetch(i).wait()
    begin(weights[:3])
    _norm(x_s, gain_ref, a_s)
    begin(weights[3:])

    @pl.when(i + 1 < pl.num_programs(0))
    def _():
        fetch(i + 1).start()

    def project(r):
        return _dot(a_s[...], wq_s[:, pl.ds(pl.multiple_of(r * PANEL, PANEL), PANEL)]).astype(jnp.bfloat16)

    def turn(t, r):
        for n in range(2):
            q_s[lax.rem(r, 2), n] = _rotate(t[:, n * HEAD : (n + 1) * HEAD], cos_ref[...], sin_ref[...])

    def attend(r, beside):
        heads = [2 * r + n for n in range(2)]
        kv = [lax.div(head, group) for head in heads]
        scores = [_scores(q_s[lax.rem(r, 2), n], k_s[kv[n]]) for n in range(2)]
        got = beside()
        for n in range(2):
            _weigh(scores[n], vt_s[kv[n]], seen_s, pl.multiple_of(heads[n] * HEAD, HEAD))
        return got

    for n in range(3):
        ready(n)
    t = _dot(a_s[...], wk_s[...]).astype(jnp.bfloat16)
    for n in range(kvs):
        k_s[n] = _rotate(t[:, n * HEAD : (n + 1) * HEAD], cos_ref[...], sin_ref[...])
    t = _dot(a_s[...], wv_s[...])
    for n in range(kvs):
        vt_s[n, :HEAD, :] = t[:, n * HEAD : (n + 1) * HEAD].T.astype(jnp.bfloat16)
        vt_s[n, HEAD:, :] = jnp.ones((16, tokens), jnp.bfloat16)
    turn(project(0), 0)
    ready(3)

    def both(r, _):
        turn(attend(r, lambda: project(r + 1)), r + 1)
        return _

    lax.fori_loop(0, nq - 1, both, None)
    attend(jnp.int32(nq - 1), lambda: None)
    for n in range(no):
        ready(4 + n)
    for n in range(no):
        o_ref = send_ref if n < per else keep_ref
        o_ref[:, n % per * PIECE : (n % per + 1) * PIECE] = _dot(seen_s[...], wo_s[n]).astype(jnp.bfloat16)


def attention_half(token, core, x, gain, cos, sin, wk, wv, wq, wo, first, count):
    _, tokens, d = x.shape
    qd, kvd, half = wq.shape[1], wk.shape[1], d // 2
    no = d // PIECE
    whole = lambda i, core: (0, 0)
    out = jax.ShapeDtypeStruct((count * tokens, half), jnp.bfloat16)
    rows = pl.BlockSpec((tokens, half), lambda i, core: (i, 0))
    return _call(
        functools.partial(_attention_kernel, first=first, group=qd // kvd), token, (core, x, gain, cos, sin, wk, wv, wq, wo), (count,),
        in_specs=[ANY, _once((1, d), whole), _once((tokens, HEAD), whole), _once((tokens, HEAD), whole), ANY, ANY, ANY, ANY],
        out_specs=[rows, rows],
        out_shape=[out, out],
        scratch=[
            pltpu.VMEM((tokens, d), jnp.bfloat16),
            pltpu.VMEM((tokens, d), jnp.bfloat16),
            pltpu.VMEM((2, 2, tokens, HEAD), jnp.bfloat16),
            pltpu.VMEM((kvd // HEAD, tokens, HEAD), jnp.bfloat16),
            pltpu.VMEM((kvd // HEAD, HEAD + 16, tokens), jnp.bfloat16),
            pltpu.VMEM((tokens, qd), jnp.bfloat16),
            pltpu.VMEM((d, kvd), jnp.bfloat16),
            pltpu.VMEM((d, kvd), jnp.bfloat16),
            pltpu.VMEM((d, qd), jnp.bfloat16),
            pltpu.VMEM((no, qd, PIECE), jnp.bfloat16),
            pltpu.SemaphoreType.DMA,
            pltpu.SemaphoreType.DMA((4 + no,)),
        ],
        cost=pl.CostEstimate(
            flops=count * (2 * tokens * d * (2 * qd + 2 * kvd) + 4 * tokens * tokens * qd),
            transcendentals=count * tokens * tokens * qd // HEAD,
            bytes_accessed=2 * (2 * count * tokens * d + d * (2 * qd + 2 * kvd))),
    )


def _mlp_kernel(core_ref, *refs, nf, pieces, count, hidden_in, hidden_out):
    given, refs = (refs[:1], refs[1:]) if hidden_in else (refs[: 2 * count], refs[2 * count :])
    (gain_ref, wg_hbm, wu_hbm), refs = ((None,) * 3, refs) if hidden_in else (refs[:3], refs[3:])
    wd_hbm, refs = refs[0], refs[1:]
    outs, refs = refs[: 2 * count], refs[2 * count :]
    hid_hbm, refs = (refs[0], refs[1:]) if hidden_out else (None, refs)
    w_s, b_s, hid_s, t_s, w_sem, h_sem, t_sem = (refs[0], None, *refs[1:]) if hidden_in else refs
    half = wd_hbm.shape[1] // 2
    per, last = len(pieces), nf + len(pieces)
    seq, j = lax.div(pl.program_id(0), last), lax.rem(pl.program_id(0), last)

    def slot(i, step):
        return 2 * lax.rem(step, 2) + i

    def gate_up(i, step):
        src, at = (wg_hbm, wu_hbm)[i], slot(i, step)
        column = pl.multiple_of(step * WIDE, WIDE)
        return pltpu.make_async_copy(src.at[:, pl.ds(column, WIDE)], w_s.at[at, pl.ds(0, src.shape[0]), :], w_sem.at[at])

    def down(i, step):
        q, at = 2 * (step - nf) + i, slot(i, step)
        core = jnp.where(q < per, 1 - core_ref[0], core_ref[0])
        column = pl.multiple_of(core * half + (lax.rem(q, per) + pieces[0]) * COLS, COLS)
        return pltpu.make_async_copy(wd_hbm.at[:, pl.ds(column, COLS)], w_s.at[at, :, pl.ds(0, COLS)], w_sem.at[at])

    def start(step):
        if nf:
            @pl.when(step < nf)
            def _():
                for i in range(2):
                    gate_up(i, step).start()

        @pl.when((step >= nf) & (step < last))
        def _():
            for i in range(2):
                down(i, step).start()

    def out(q, begin):
        to, at = pl.multiple_of(lax.rem(q, per) * COLS, COLS), lax.rem(q, 4)
        for n, ref in enumerate(outs):
            @pl.when((seq == n // 2) & ((q >= per) if n % 2 else (q < per)))
            def _():
                copy = pltpu.make_async_copy(t_s.at[at], ref.at[:, pl.ds(to, COLS)], t_sem.at[at])
                copy.start() if begin else copy.wait()

    def fetch(n):
        starts = [pl.multiple_of(core * half, 128) for core in (core_ref[0], 1 - core_ref[0])]
        return [pltpu.make_async_copy(ref, b_s.at[:, pl.ds(at, half)], h_sem.at[k])
                for k, (ref, at) in enumerate(zip(given[2 * n : 2 * n + 2], starts))]

    if hidden_in:

        @pl.when(j == 0)
        def _():
            copy = pltpu.make_async_copy(given[0], hid_s, h_sem.at[0])
            copy.start()
            down(0, j).start()
            copy.wait()
            down(1, j).start()
    else:
        for n in range(count):

            @pl.when((seq == n) & (j == 0))
            def _():
                for copy in fetch(n):
                    if n == 0:
                        copy.start()
                for copy in fetch(n):
                    copy.wait()
                if n == 0:
                    start(j)
                _norm(b_s, gain_ref, b_s)

            if n + 1 < count:

                @pl.when((seq == n) & (j == nf))
                def _():
                    for copy in fetch(n + 1):
                        copy.start()

                @pl.when((seq == n) & (j == last - 1))
                def _():
                    start(jnp.int32(0))

    start(j + 1)

    if nf:
        @pl.when(j < nf)
        def _():
            for i in range(2):
                gate_up(i, j).wait()
            d = b_s.shape[1]
            for p in range(WIDE // PANEL):
                at = slice(p * PANEL, (p + 1) * PANEL)
                gate = _dot(b_s[...], w_s[slot(0, j), :d, at])
                up = _dot(b_s[...], w_s[slot(1, j), :d, at])
                to = pl.ds(pl.multiple_of(j * WIDE + p * PANEL, PANEL), PANEL)
                hid_s[:, to] = (gate * jax.nn.sigmoid(gate) * up).astype(jnp.bfloat16)

    if hidden_out:
        put = pltpu.make_async_copy(hid_s, hid_hbm, h_sem.at[0])

        @pl.when(j == nf)
        def _():
            put.start()

    @pl.when(j >= nf)
    def _():
        q = 2 * (j - nf)

        @pl.when(q >= 4)
        def _():
            for i in range(2):
                out(q - 4 + i, False)

        if not hidden_in:
            for i in range(2):
                down(i, j).wait()
        for i in range(2):
            if hidden_in:
                down(i, j).wait()
            t_s[lax.rem(q + i, 4)] = _dot(hid_s[...], w_s[slot(i, j), :, :COLS]).astype(jnp.bfloat16)
        for i in range(2):
            out(q + i, True)

        @pl.when(j == last - 1)
        def _():
            for i in range(-2, 2):
                out(q + i, False)
            if hidden_out:
                put.wait()


def mlp(token, core, given, weights, wd, pieces, hidden_out=False):
    ff, d = wd.shape
    tokens, hidden_in, count = 512, not weights, max(len(given) // 2, 1)
    per = len(pieces)
    nf = 0 if hidden_in else ff // WIDE
    out = jax.ShapeDtypeStruct((tokens, per * COLS), jnp.bfloat16)
    hidden = jax.ShapeDtypeStruct((tokens, ff), jnp.bfloat16)
    flops = count * ((0 if hidden_in else 4 * tokens * d * ff) + 2 * tokens * ff * 2 * per * COLS)
    return _call(
        functools.partial(_mlp_kernel, nf=nf, pieces=pieces, count=count, hidden_in=hidden_in, hidden_out=hidden_out), token,
        (core, *given, *weights, wd), (count * (nf + per),),
        in_specs=[ANY] * len(given) + ([] if hidden_in else [_once((1, d), lambda j, core: (0, 0)), ANY, ANY]) + [ANY],
        out_specs=[ANY] * (2 * count + hidden_out),
        out_shape=[out] * 2 * count + [hidden] * hidden_out,
        scratch=[pltpu.VMEM((4, ff, COLS if hidden_in else WIDE), jnp.bfloat16)]
        + [pltpu.VMEM((tokens, d), jnp.bfloat16)] * (not hidden_in)
        + [
            pltpu.VMEM((tokens, ff), jnp.bfloat16),
            pltpu.VMEM((4, tokens, COLS), jnp.bfloat16),
            pltpu.SemaphoreType.DMA((4,)),
            pltpu.SemaphoreType.DMA((2,)),
            pltpu.SemaphoreType.DMA((4,)),
        ],
        cost=pl.CostEstimate(flops=flops, transcendentals=count * tokens * ff, bytes_accessed=flops // tokens + 4 * count * tokens * d),
    )


def _sums_kernel(core_ref, *refs, jobs, count, fresh, aliased):
    arrays, refs = refs[:count], refs[count:]
    made, refs = refs[: fresh], refs[fresh:]
    y_hbm, refs = (refs[0], refs[1:]) if aliased else (None, refs)
    core = core_ref[0]
    rows = 64
    todo = []
    at_array = at_made = 0
    for seq, terms, keep, to, size, wide in jobs:
        sem, osem, o_s, *t_s = refs[: 3 + len(terms)]
        refs = refs[3 + len(terms) :]
        held = arrays[at_array : at_array + len(terms)]
        at_array += len(terms)
        out = made[at_made] if keep else None
        at_made += bool(keep)
        for r in range(size // rows):
            here = pl.ds(r * rows, rows)
            ins, outs = [], []
            for n, ((row, column), array) in enumerate(zip(terms, held)):
                if len(array.shape) == 3:
                    half = array.shape[2] // 2
                    src = array.at[seq + r * rows // 512, pl.ds(r * rows % 512, rows), pl.ds(pl.multiple_of(core * half, 128), wide)]
                else:
                    src = array.at[pl.ds(row + r * rows, rows), pl.ds(column, wide)]
                ins.append(pltpu.make_async_copy(src, t_s[n].at[here], sem.at[n, r]))
            from_s = o_s if len(terms) > 1 else t_s[0]
            if keep:
                outs.append(pltpu.make_async_copy(from_s.at[here], out.at[here], osem.at[0, r]))
            if to is not None:
                mine, column = to
                half = y_hbm.shape[2] // 2
                start = pl.multiple_of((core if mine else 1 - core) * half + column, 128)
                outs.append(pltpu.make_async_copy(from_s.at[here], y_hbm.at[seq, here, pl.ds(start, wide)], osem.at[1, r]))

            def work(o_s=o_s, t_s=t_s, first=r * rows, rows=rows):
                def some(k, _):
                    at = pl.ds(pl.multiple_of(first + k * 16, 16), 16)
                    for c in range(0, o_s.shape[1], COLS):
                        total = None
                        for t in t_s[::-1]:
                            t = t[at, c : c + COLS].astype(jnp.float32)
                            total = t if total is None else t + total
                        o_s[at, c : c + COLS] = total.astype(jnp.bfloat16)
                    return _

                if len(t_s) > 1:
                    lax.fori_loop(0, rows // 16, some, None)

            todo.append((ins, outs, work))
    for ins, _, _ in todo:
        for copy in ins:
            copy.start()
    for ins, outs, work in todo:
        for copy in ins:
            copy.wait()
        work()
        for copy in outs:
            copy.start()
    for _, outs, _ in todo:
        for copy in outs:
            copy.wait()


def sums(token, core, jobs, y=None, shape=None):
    given, plain, scratch, out_shape, work = [], [], [], [], 0
    for seq, terms, keep, to in jobs:
        terms = [(t + (0, 0))[:3] for t in terms]
        size, wide = terms[-1][0].shape
        size = min(size, 512)
        given += [t[0] for t in terms]
        plain.append((seq, [t[1:] for t in terms], keep, to, size, wide))
        buffer = pltpu.VMEM((size, wide), jnp.bfloat16)
        scratch += [pltpu.SemaphoreType.DMA((len(terms), size // 64)), pltpu.SemaphoreType.DMA((2, size // 64))]
        scratch += [buffer if len(terms) > 1 else pltpu.VMEM((16, 128), jnp.bfloat16)] + [buffer] * len(terms)
        out_shape += [jax.ShapeDtypeStruct((size, wide), jnp.bfloat16)] * bool(keep)
        work += (len(terms) + 1) * size * wide
    count, fresh = len(given), len(out_shape)
    aliased = any(to is not None for *_, to in jobs)
    if aliased:
        out_shape.append(jax.ShapeDtypeStruct(shape, jnp.bfloat16))
    had = aliased and y is not None

    def kernel(core_ref, *refs):
        _sums_kernel(core_ref, *refs[:count], *refs[count + had :], jobs=plain, count=count, fresh=fresh, aliased=aliased)

    out, token = _call(
        kernel, token, (core, *given, *([y] if had else [])), (1,),
        in_specs=[ANY] * (count + had),
        out_specs=[ANY] * len(out_shape),
        out_shape=out_shape,
        scratch=scratch,
        aliases={1 + count: fresh} if had else None,
        cost=pl.CostEstimate(flops=work, transcendentals=0, bytes_accessed=2 * work),
    )
    return tuple(out), token


def solution(mesh):
    n = mesh.shape["tp"]
    core_pairs = [(i, i ^ 1) for i in range(n)]
    chip_pairs = [(i, i ^ 2) for i in range(n)]

    def step(x, gain_a, wq, wk, wv, wo, gain_m, w_gate, w_up, w_down):
        tokens, d = x.shape[1:]
        core = lax.rem(lax.axis_index("tp"), 2).reshape(1)
        angle = jnp.arange(tokens, dtype=jnp.float32)[:, None] * THETA ** (-(jnp.arange(HEAD) % (HEAD // 2)).astype(jnp.float32) / (HEAD // 2))
        cos, sin = jnp.cos(angle), jnp.sin(angle) * jnp.where(jnp.arange(HEAD) < HEAD // 2, -1.0, 1.0)
        gain_a, gain_m = gain_a.reshape(1, d), gain_m.reshape(1, d)
        token, y = cos, None

        def run(f, *args, **more):
            nonlocal token
            out, token = f(token, core, *args, **more)
            return out

        def send(pairs, array):
            return lax.ppermute(array, "tp", pairs)

        def attention(s, count=1):
            out, keep = run(attention_half, x, gain_a, cos, sin, wk, wv, wq, wo, s, count)
            return send(core_pairs, out), keep

        def gated(given, pieces, **more):
            out = run(mlp, given, weights, w_down, pieces, **more)
            return (send(core_pairs, out[0]), *out[1:])

        def chip_sum(came, keep):
            (term,) = run(sums, [(0, [(keep,), (came,)], True, None)])
            return term, send(chip_pairs, term)

        def residual(s, term, came):
            (own,) = run(sums, [(s, [(x,), (term,), (came,)], True, None)])
            return own, send(core_pairs, own)

        def finish(s, base, column, term, came, others=()):
            nonlocal y
            mine = (s, [base, (term,), (came,)], True, (True, column))
            own, y = run(sums, [mine, *others], y, x.shape)
            return send(core_pairs, own)

        def put(s, came, column=0):
            return s, [(came,)], False, (False, column)

        weights = gain_m, w_gate, w_up
        every = tuple(range(d // 2 // COLS))
        cut = 3
        a0 = attention(0)
        a1 = attention(1)
        a0 = chip_sum(*a0)
        came, keep = attention(2, 2)
        a1 = chip_sum(*a1)
        h0 = residual(0, *a0)
        a2, a3 = run(sums, [(0, [(keep, n * tokens), (came, n * tokens)], True, None) for n in range(2)])
        a2, a3 = (a2, send(chip_pairs, a2)), (a3, send(chip_pairs, a3))
        m0 = gated(h0, every)
        h1 = residual(1, *a1)
        h2 = residual(2, *a2)
        m0 = chip_sum(*m0)
        out = run(mlp, (*h1, *h2), weights, w_down, every)
        m1, m2 = (send(core_pairs, out[0]), out[1]), (send(core_pairs, out[2]), out[3])
        h3 = residual(3, *a3)
        m1 = chip_sum(*m1)
        m2 = chip_sum(*m2)
        *m3, hidden = gated(h3, every[:cut], hidden_out=True)
        m3 = chip_sum(*m3)
        came = run(mlp, (hidden,), (), w_down, every[cut:])
        m4 = send(core_pairs, came[0]), came[1]
        r0 = finish(0, (h0[0],), 0, *m0)
        m4 = chip_sum(*m4)
        r1 = finish(1, (h1[0],), 0, *m1)
        r2 = finish(2, (h2[0],), 0, *m2)
        y = run(sums, [put(0, r0), put(1, r1)], y, x.shape)[0]
        r3 = finish(3, (h3[0],), 0, *m3, [put(2, r2)])
        r4 = finish(3, (h3[0], 0, cut * COLS), cut * COLS, *m4)
        return run(sums, [put(3, r3), put(3, r4, cut * COLS)], y, x.shape)[0]

    tokens, whole, columns, rows_of = P("dp", None, None), P(None), P(None, "tp"), P("tp", None)
    return jax.shard_map(
        step,
        mesh=mesh,
        in_specs=(tokens, whole, columns, columns, columns, rows_of, whole, columns, columns, rows_of),
        out_specs=tokens,
        check_vma=False,
    )
```
